32 devices in a mesh: dp: 16 (over z, y, core), rep: 2 (over x).
Axes of the slice: x: 2, y: 2, z: 4, core: 2. Of those that a mesh axis runs over, the one named last changes fastest.
Arguments:
- q_hidden: bfloat16 [2, 16, 128, 768], P('rep', 'dp'), may hold values from -8 to 8
- p_hidden: bfloat16 [2, 16, 128, 768], P('rep', 'dp'), may hold values from -8 to 8
- w_up: bfloat16 [1536, 768], replicated, may hold values from -0.21875 to 0.21875
- w_down: bfloat16 [1536, 768], replicated, may hold values from -0.15625 to 0.15625
- pos_index: int32 [2, 16], P('rep', 'dp'), may hold values from 0 to 15
- hard_index: int32 [2, 16, 2], P('rep', 'dp'), may hold values from 0 to 15
Outputs:
- w_up_grad: float32 [1536, 768], P(('dp', 'rep'))
- mean_loss: float32 [], replicated
The draws below stay inside these ranges and needn't reach their ends.
All inputs are finite; a program needn't handle non-finite values.
Results may differ from the reference program's by a relative error of at most 0.008.
Values may be sent and summed in bfloat16 or wider, within the bound.
A program may use at most 64 MiB of HBM per device.

```python
import math
import jax
import jax.numpy as jnp
from jax import lax

D = 768
FF = 1536
LEN = 128
HARD = 2
REPLICAS = 2
GQ = 16
GP = 16


def hidden_pair(key):
    shape = (2, REPLICAS, GQ, LEN, D)
    topic = jax.random.normal(jax.random.fold_in(key, 101), (2, REPLICAS, GQ, 1, D), jnp.float32)
    noise = jax.random.normal(jax.random.fold_in(key, 202), shape, jnp.float32)
    both = 0.35 * topic + noise
    return jnp.clip(both, -8.0, 8.0)


def draw_q_hidden(key, part):
    return hidden_pair(key)[0].astype(jnp.bfloat16)


def draw_p_hidden(key, part):
    return hidden_pair(key)[1].astype(jnp.bfloat16)


def place_ends(array, stream_key, low, top_value):
    dims = array.shape
    spot = [jax.random.randint(jax.random.fold_in(stream_key, axis), (), 0, dims[axis]) for axis in range(len(dims))]
    array = array.at[tuple(spot)].set(low)
    longest = dims.index(max(dims))
    spot[longest] = (spot[longest] + 1) % dims[longest]
    return array.at[tuple(spot)].set(top_value)


def normal_values(rng, shape, width, reach, kind=jnp.bfloat16):
    return jnp.clip(width * jax.random.normal(rng, shape, jnp.float32), -reach, reach).astype(kind)


def setup_inputs(seed: int = 0) -> dict:
    keys = jax.random.split(jax.random.key(seed), 7)
    return {
        "q_hidden": draw_q_hidden(jax.random.fold_in(keys[6], 71), 0),
        "p_hidden": draw_p_hidden(jax.random.fold_in(keys[6], 71), 0),
        "w_up": normal_values(keys[2], (FF, D), D ** -0.5, 0.21875),
        "w_down": normal_values(keys[3], (FF, D), FF ** -0.5, 0.15625),
        "pos_index": place_ends(jax.random.randint(keys[4], (REPLICAS, GQ), 0, GP), jax.random.fold_in(keys[4], 1), 0, GP - 1).astype(jnp.int32),
        "hard_index": place_ends(jax.random.randint(keys[5], (REPLICAS, GQ, HARD), 0, GP), jax.random.fold_in(keys[5], 1), 0, GP - 1).astype(jnp.int32),
    }


norm_eps = 1e-06
HARD_BOOST = 1.5

def gelu_slope(values):
    cdf_part = 0.5 * (1.0 + lax.erf(values * (1.0 / math.sqrt(2.0))))
    return cdf_part + values * jnp.exp(-0.5 * values * values) * (1.0 / math.sqrt(2.0 * math.pi))

def encode(seq_block, w_up, w_down):
    tokens = seq_block.reshape(-1, seq_block.shape[-1])
    pre_act = jnp.dot(tokens, w_up.T, preferred_element_type=jnp.float32)
    hidden = jax.nn.gelu(pre_act, approximate=False).astype(jnp.bfloat16)
    summed = tokens.astype(jnp.float32) + jnp.dot(hidden, w_down, preferred_element_type=jnp.float32)
    row_mean = lax.optimization_barrier(jnp.mean(summed, -1, keepdims=True))
    centred = summed - row_mean
    inv_scale = lax.rsqrt(lax.optimization_barrier(jnp.mean(centred * centred, -1, keepdims=True)) + norm_eps)
    normed = centred * inv_scale
    return (tokens, pre_act, hidden, normed, inv_scale)

def backward(pre_act, normed, inv_scale, d_embed, length, w_down):
    grad_out = jnp.repeat(d_embed / length, length, axis=0)
    grad_resid = inv_scale * (grad_out - lax.optimization_barrier(jnp.mean(grad_out, -1, keepdims=True)) - normed * lax.optimization_barrier(jnp.mean(grad_out * normed, -1, keepdims=True)))
    grad_low = grad_resid.astype(jnp.bfloat16)
    grad_hidden = jnp.dot(grad_low, w_down.T, preferred_element_type=jnp.float32)
    grad_pre = (grad_hidden * gelu_slope(pre_act)).astype(jnp.bfloat16)
    return (grad_low, grad_pre)

def reference(q_hidden, p_hidden, w_up, w_down, pos_index, hard_index):
    block_rows = 8
    every_seq = jnp.concatenate([q_hidden.reshape(-1, LEN, D), p_hidden.reshape(-1, LEN, D)], 0)
    blocks = every_seq.reshape(-1, block_rows, LEN, D)

    def embed(seq_block):
        normed = encode(seq_block, w_up, w_down)[3]
        return lax.optimization_barrier(jnp.mean(normed.reshape(block_rows, LEN, D), 1)).astype(jnp.bfloat16)
    embedded = lax.map(embed, blocks).reshape(2, REPLICAS, GQ, D)
    query_embed = embedded[0]
    passage_embed = embedded[1]
    scores = jnp.einsum('rqd,rpd->rqp', query_embed.astype(jnp.float32), passage_embed.astype(jnp.float32))
    columns = jnp.arange(GP, dtype=jnp.int32)
    hard_mask = jnp.any(hard_index[..., None] == columns, axis=-2)
    logits = scores + HARD_BOOST * hard_mask.astype(jnp.float32)
    row_max = lax.optimization_barrier(jnp.max(logits, -1, keepdims=True))
    log_total = row_max + jnp.log(lax.optimization_barrier(jnp.sum(jnp.exp(logits - row_max), -1, keepdims=True)))
    target = pos_index[..., None] == columns
    picked = lax.optimization_barrier(jnp.sum(jnp.where(target, logits, 0.0), -1))
    loss_sum = jnp.sum(log_total[..., 0] - picked)
    weights = (jnp.exp(logits - log_total) - target.astype(jnp.float32)).astype(jnp.bfloat16)
    d_query = jnp.einsum('rqp,rpd->rqd', weights.astype(jnp.float32), passage_embed.astype(jnp.float32))
    d_passage = jnp.einsum('rqp,rqd->rpd', weights.astype(jnp.float32), query_embed.astype(jnp.float32))
    d_all = jnp.concatenate([d_query.reshape(-1, D), d_passage.reshape(-1, D)], 0).reshape(-1, block_rows, D)

    def accumulate(up_sum, items):
        seq_block, d_embed = items
        tokens, pre_act, hidden, normed, inv_scale = encode(seq_block, w_up, w_down)
        grad_low, grad_pre = backward(pre_act, normed, inv_scale, d_embed, LEN, w_down)
        up_sum = up_sum + jnp.dot(grad_pre.T, tokens, preferred_element_type=jnp.float32)
        return (up_sum, None)
    up_sum, unused = lax.scan(accumulate, jnp.zeros((FF, D), jnp.float32), (blocks, d_all))
    return (up_sum, loss_sum / (REPLICAS * GQ))
```

```python
import functools
import math

import jax
import jax.numpy as jnp
from jax import lax
from jax.experimental import pallas as pl
from jax.experimental.pallas import tpu as pltpu
from jax.sharding import PartitionSpec as P

norm_eps = 1e-06
HARD_BOOST = 1.5
MESH = pl.DeviceIdType.MESH
LANES = 128
ROW_TILE = 16
F32 = jnp.float32
BF16 = jnp.bfloat16


def dot_nt(left, right):
    return lax.dot_general(
        left, right, (((1,), (1,)), ((), ())), preferred_element_type=F32
    )


def phi(values):
    return 0.5 * (1.0 + lax.erf(values * (1.0 / math.sqrt(2.0))))


def gelu_slope(values):
    bell = jnp.exp(-0.5 * values * values) * (1.0 / math.sqrt(2.0 * math.pi))
    return phi(values) + values * bell


def loop(count, body):
    if count <= 16:
        for step in range(count):
            body(step)
    else:
        lax.fori_loop(0, count, lambda step, carry: (body(step), carry)[1], 0)


def kernel(
    dp, rep, pairs, length, hard,
    q_ref, p_ref, up_ref, down_ref, pos_ref, hard_ref,
    out_ref, loss_ref,
    up, down, tokens, hidden, slope, normed, inv_scale, grad_low, slots, index_slots, every,
    index_rows, gp_send, gp_recv, halves, kept, y_out, y_in, z_out, z_in, losses,
    pos_smem, hard_smem, t_sem, w_sem, x_send, x_recv, f_send, f_recv, i_send, i_recv, e_send, e_recv,
    l_send, l_recv, g_send, g_recv, y_send, y_recv, z_send, z_recv, below, above,
):
    depth = dp // 4
    members = 2 * rep
    seqs = 2 * pairs
    count = seqs * length
    features = tokens.shape[-1]
    rows = up.shape[-2]
    chunk = members * 2 * rows
    strips = rows // ROW_TILE
    padded = every.shape[0]
    me = lax.axis_index("dp")
    my_rep = lax.axis_index("rep")
    core = lax.rem(me, 2)
    side = lax.rem(me // 2, 2)
    layer = me // 4
    member = core * rep + my_rep
    partner = me + 1 - 2 * core

    def remote(src, dst, send, recv, device):
        return pltpu.make_async_remote_copy(
            src_ref=src, dst_ref=dst, send_sem=send, recv_sem=recv,
            device_id=device, device_id_type=MESH,
        )

    def ahead(step):
        return lax.rem(me + step, dp)

    def behind(step):
        return lax.rem(me + dp - step, dp)

    def rep_ahead(step):
        return lax.rem(my_rep + step, rep)

    def rep_behind(step):
        return lax.rem(my_rep + rep - step, rep)

    half = pairs * length
    load_q = pltpu.make_async_copy(q_ref, tokens.at[member, pl.ds(0, half)], t_sem.at[0])
    load_p = pltpu.make_async_copy(p_ref, tokens.at[member, pl.ds(half, half)], t_sem.at[1])
    load_q.start()
    load_p.start()
    load_pos = pltpu.make_async_copy(pos_ref, pos_smem, t_sem.at[2])
    load_hard = pltpu.make_async_copy(hard_ref, hard_smem, t_sem.at[3])

    def load(which, step, part):
        ref, buffer = ((up_ref, up), (down_ref, down))[which]
        return pltpu.make_async_copy(
            ref.at[step, part], buffer.at[step, :, part], w_sem.at[which, step]
        )

    def load_chunk(step):
        for which in range(2):
            for part in range(2):
                load(which, step, part).start()

    loop(depth, load_chunk)
    load_pos.start()
    load_hard.start()

    barrier = pltpu.get_barrier_semaphore()

    opposite = me + 2 - 4 * side

    def greet(device, group):
        pl.semaphore_signal(
            barrier, inc=1, device_id=(device, group), device_id_type=MESH
        )

    greet(partner, my_rep)
    for step in range(1, rep):
        greet(me, rep_ahead(step))
        greet(partner, rep_ahead(step))
    greet(opposite, my_rep)
    greet(opposite + partner - me, my_rep)

    @pl.when(layer + 1 < depth)
    def greet_above():
        greet(me + 4, my_rep)

    @pl.when(layer > 0)
    def greet_below():
        greet(me - 4, my_rep)

    def wait_near():
        pl.semaphore_wait(
            barrier,
            3 + 2 * (rep - 1) + jnp.where(layer + 1 < depth, 1, 0) + jnp.where(layer > 0, 1, 0),
        )

    def hear(step):
        @pl.when(layer >= step)
        def from_below():
            pl.semaphore_wait(below, 1)

        @pl.when(layer + step < depth)
        def from_above():
            pl.semaphore_wait(above, 1)

    def tell(step):
        @pl.when((layer >= step) & (layer + 1 < depth))
        def to_above():
            pl.semaphore_signal(below, inc=1, device_id=(me + 4, my_rep), device_id_type=MESH)

        @pl.when((layer + step < depth) & (layer > 0))
        def to_below():
            pl.semaphore_signal(above, inc=1, device_id=(me - 4, my_rep), device_id_type=MESH)

    def spread(step):
        hear(step)
        if depth <= 16:
            if step < depth - 1:
                tell(step)
        else:
            pl.when(step < depth - 1)(lambda: tell(step))

    every[...] = jnp.zeros_like(every)
    index_rows[...] = jnp.full(index_rows.shape, -1, jnp.int32)

    load_q.wait()
    load_p.wait()
    own = tokens[member]

    def wait_weights(which, step):
        buffer = (up, down)[which].at[step]
        pltpu.make_async_copy(buffer, buffer, w_sem.at[which, step]).wait()

    def forward(step):
        wait_weights(0, step)
        pre = dot_nt(own, up[step].reshape(chunk, features))
        columns = pl.ds(pl.multiple_of(step * chunk, chunk), chunk)
        hidden[:, columns] = (pre * phi(pre)).astype(BF16)

    forward(0)
    load_pos.wait()
    load_hard.wait()
    row_ids = lax.broadcasted_iota(jnp.int32, (seqs, LANES), 0)
    lane_ids = lax.broadcasted_iota(jnp.int32, (seqs, LANES), 1)
    message = jnp.full((seqs, LANES), -1, jnp.int32)
    for row in range(pairs):
        message = jnp.where((row_ids == row) & (lane_ids == 0), pos_smem[0, row], message)
        for pick in range(hard):
            message = jnp.where(
                (row_ids == row) & (lane_ids == 1 + pick), hard_smem[row, pick], message
            )
    index_slots[me] = message
    wait_near()
    tell(0)

    def x_copy(step):
        if step == 0:
            device = (partner, my_rep)
        else:
            device = (me, rep_ahead(step))
        return remote(
            tokens.at[member], tokens.at[member], x_send.at[step], x_recv.at[step], device
        )

    for step in range(rep - 1, -1, -1):
        x_copy(step).start()

    def index_copy(step):
        return remote(
            index_slots.at[me], index_slots.at[me], i_send.at[0], i_recv.at[0],
            (ahead(step + 1), my_rep),
        )

    def forward_and_spread(step):
        forward(step + 1)
        spread(step + 1)

    loop(depth - 1, forward_and_spread)
    loop(dp - 1, lambda step: index_copy(step).start())
    loop(depth, lambda step: wait_weights(1, step))
    summed = own.astype(F32) + jnp.dot(
        hidden[...], down[...].reshape(depth * chunk, features), preferred_element_type=F32
    )

    means = []
    for seq in range(seqs):
        block = summed[seq * length:(seq + 1) * length]
        centred = block - jnp.mean(block, -1, keepdims=True)
        scale = lax.rsqrt(jnp.mean(centred * centred, -1, keepdims=True) + norm_eps)
        unit = centred * scale
        inv_scale[pl.ds(seq * length, length), :] = scale
        normed[pl.ds(seq * length, length), :] = unit
        means.append(jnp.mean(unit, 0, keepdims=True))
    slots[me] = jnp.concatenate(means, 0).astype(BF16)

    def embed_copy(step):
        return remote(
            slots.at[me], slots.at[me], e_send.at[0], e_recv.at[0],
            (ahead(step + 1), my_rep),
        )

    loop(dp - 1, lambda step: embed_copy(step).start())

    def keep_slope(step):
        pre = dot_nt(up[step].reshape(chunk, features), own)
        bell = jnp.exp(-0.5 * pre * pre) * (1.0 / math.sqrt(2.0 * math.pi))
        slope[step] = phi(pre) + pre * bell

    loop(depth, keep_slope)

    def all_indices():
        landed = index_slots.at[pl.ds(0, dp - 1)]
        return remote(landed, landed, i_send.at[0], i_recv.at[0], (me, my_rep))

    def all_embeds():
        landed = slots.at[pl.ds(0, dp - 1)]
        return remote(landed, landed, e_send.at[0], e_recv.at[0], (me, my_rep))

    all_indices().wait_recv()
    all_embeds().wait_recv()
    for slot in range(dp):
        every[slot * seqs:(slot + 1) * seqs, :] = slots[slot].astype(F32)
        index_rows[slot * seqs:(slot + 1) * seqs, :] = index_slots[slot]

    embeds = every[...].astype(BF16)
    scores = dot_nt(embeds, embeds)
    row = lax.broadcasted_iota(jnp.int32, (padded, padded), 0)
    column = lax.broadcasted_iota(jnp.int32, (padded, padded), 1)
    row_place = lax.rem(row, seqs)
    column_place = lax.rem(column, seqs)
    valid = (
        (row < dp * seqs) & (row_place < pairs) & (column < dp * seqs) & (column_place >= pairs)
    )
    passage = (column // seqs) * pairs + column_place - pairs
    indices = index_rows[...]
    target = valid & (passage == indices[:, 0:1])
    is_hard = passage == indices[:, 1:2]
    for pick in range(1, hard):
        is_hard = is_hard | (passage == indices[:, 1 + pick:2 + pick])
    logits = scores + jnp.where(is_hard, HARD_BOOST, 0.0)
    row_max = jnp.max(jnp.where(valid, logits, -1e30), -1, keepdims=True)
    powers = jnp.where(valid, jnp.exp(jnp.where(valid, logits - row_max, 0.0)), 0.0)
    powers_sum = jnp.sum(powers, -1, keepdims=True)
    log_total = row_max + jnp.log(jnp.where(powers_sum > 0.0, powers_sum, 1.0))
    picked = jnp.sum(jnp.where(target, logits, 0.0), -1, keepdims=True)
    weights = jnp.where(
        valid,
        jnp.exp(jnp.where(valid, logits - log_total, 0.0)) - jnp.where(target, 1.0, 0.0),
        0.0,
    )
    both = weights + weights.T
    own_weights = [
        jnp.sum(jnp.where(row == me * seqs + seq, both, 0.0), 0, keepdims=True)
        for seq in range(seqs)
    ]
    own_weights = jnp.concatenate(own_weights, 0).astype(BF16)
    d_own = jnp.dot(own_weights, embeds, preferred_element_type=F32) * (1.0 / length)
    row_one = lax.broadcasted_iota(jnp.int32, (padded, 1), 0)
    counted = (row_one < dp * seqs) & (lax.rem(row_one, seqs) < pairs)
    loss = jnp.sum(jnp.where(counted, log_total - picked, 0.0), 0, keepdims=True)
    losses[my_rep] = jnp.broadcast_to(loss, (1, LANES))

    def loss_copy(step):
        return remote(
            losses.at[my_rep], losses.at[my_rep], l_send.at[step], l_recv.at[step],
            (me, rep_ahead(step)),
        )

    for step in range(1, rep):
        loss_copy(step).start()

    for seq in range(seqs):
        place = pl.ds(seq * length, length)
        grad = d_own[seq:seq + 1]
        unit = normed[place, :]
        grad_low[place, :] = (
            inv_scale[place, :]
            * (
                grad
                - jnp.mean(grad, -1, keepdims=True)
                - unit * jnp.mean(grad * unit, -1, keepdims=True)
            )
        ).astype(BF16)

    def turn(step):
        own_turn = (step + 1) // depth
        upper = (2 * layer) // depth
        mirrored = upper * layer + (1 - upper) * (depth - 1 - layer)
        place = step + (step - mirrored + depth) // depth
        place = upper * place + (1 - upper) * (depth - 1 - place)
        return own_turn * layer + (1 - own_turn) * place

    def strip(sub):
        return pl.ds(sub * ROW_TILE, ROW_TILE)

    def g_copy(step, sub, jump):
        now = turn(step)
        target_member = lax.rem(member + jump, members)
        return remote(
            gp_send.at[now, target_member, :, strip(sub)],
            gp_recv.at[now, member, :, strip(sub)],
            g_send.at[0], g_recv.at[now, sub],
            (me - core + target_member // rep, lax.rem(target_member, rep)),
        )

    def backward(step):
        now = turn(step)
        grad_hidden = dot_nt(down[now].reshape(chunk, features), grad_low[...])
        grad_pre = (grad_hidden * slope[now]).astype(BF16)
        gp_send[now] = grad_pre.reshape(members, 2, rows, count)
        gp_recv[now, member] = gp_send[now, member]

    def send_grads(step):
        for sub in range(strips):
            for jump in range(1, members):
                g_copy(step, sub, jump).start()

    backward(0)
    send_grads(0)
    loop(depth - 1, lambda step: backward(step + 1))

    for step in range(1, rep):
        slot = core * rep + rep_behind(step)
        remote(
            tokens.at[slot], tokens.at[slot], x_send.at[step], x_recv.at[step],
            (me, rep_behind(step)),
        ).wait_recv()
        remote(
            tokens.at[slot], tokens.at[slot], f_send.at[step], f_recv.at[step],
            (partner, my_rep),
        ).start()
    loop(depth - 1, lambda step: send_grads(step + 1))
    slot = (1 - core) * rep + my_rep
    remote(
        tokens.at[slot], tokens.at[slot], x_send.at[0], x_recv.at[0], (partner, my_rep)
    ).wait_recv()
    for step in range(1, rep):
        slot = (1 - core) * rep + rep_behind(step)
        remote(
            tokens.at[slot], tokens.at[slot], f_send.at[step], f_recv.at[step],
            (partner, my_rep),
        ).wait_recv()

    def y_copy(now, sub):
        return remote(
            y_out.at[now, strip(sub)], y_in.at[now, strip(sub)],
            y_send.at[0], y_recv.at[now, sub],
            (me + 2 - 4 * side, my_rep),
        )

    def z_copy(now, sub):
        return remote(
            z_out.at[now, strip(sub)], z_in.at[layer, strip(sub)],
            z_send.at[0], z_recv.at[0],
            (now * 4 + side * 2 + core, my_rep),
        )

    def place_of(index):
        if strips == 1:
            return turn(index), 0
        return turn(index // strips), index % strips

    def product(index):
        now, sub = place_of(index)
        landed = gp_recv.at[now, pl.ds(0, members - 1), :, strip(sub)]
        remote(landed, landed, g_send.at[0], g_recv.at[now, sub], (me, my_rep)).wait_recv()
        total = None
        for part in range(members):
            term = jnp.dot(
                gp_recv[now, part, :, strip(sub), :].reshape(2 * ROW_TILE, count), tokens[part],
                preferred_element_type=F32,
            )
            total = term if total is None else total + term
        halves[...] = total.reshape(2, ROW_TILE, features)
        kept[now, strip(sub), :] = halves[side]
        y_out[now, strip(sub), :] = halves[1 - side].astype(BF16)
        y_copy(now, sub).start()

    def pass_on(index, last):
        now, sub = place_of(index)
        y_copy(now, sub).wait_recv()
        total = kept[now, strip(sub), :] + y_in[now, strip(sub), :].astype(F32)
        if last:
            out_ref[strip(sub), :] = total
        else:
            z_out[now, strip(sub), :] = total.astype(BF16)
            z_copy(now, sub).start()

    steps = depth * strips
    lag = 3
    moved = steps - strips
    for index in range(lag):
        product(index)

    def both_stages(index):
        product(index + lag)
        pass_on(index, False)

    paired = min(steps - lag, moved)
    loop(paired, both_stages)
    for index in range(paired, moved):
        pass_on(index, False)
    for index in range(paired + lag, steps):
        product(index)
    for index in range(moved, steps):
        pass_on(index, True)

    def all_layers():
        landed = z_in.at[pl.ds(0, depth - 1)]
        return remote(landed, landed, z_send.at[0], z_recv.at[0], (me, my_rep))

    all_layers().wait_recv()

    def collect(step):
        source = lax.rem(layer + depth - 1 - step, depth)
        out_ref[...] += z_in[source].astype(F32)

    loop(depth - 1, collect)

    for step in range(1, rep):
        source = rep_behind(step)
        remote(
            losses.at[source], losses.at[source], l_send.at[step], l_recv.at[step],
            (me, source),
        ).wait_recv()
    loss_total = losses[0]
    for part in range(1, rep):
        loss_total = loss_total + losses[part]
    loss_ref[...] = loss_total[:, 0:1] * (1.0 / (dp * pairs * rep))

    all_indices().wait_send()
    all_embeds().wait_send()
    for step in range(rep):
        x_copy(step).wait_send()
    for step in range(1, rep):
        loss_copy(step).wait_send()
        slot = core * rep + rep_behind(step)
        remote(
            tokens.at[slot], tokens.at[slot], f_send.at[step], f_recv.at[step],
            (partner, my_rep),
        ).wait_send()

    sent = gp_send.at[:, pl.ds(0, members - 1)]
    remote(sent, sent, g_send.at[0], g_recv.at[0, 0], (me, my_rep)).wait_send()
    remote(y_out, y_in, y_send.at[0], y_recv.at[0, 0], (me, my_rep)).wait_send()
    all_layers().wait_send()


def shards(dp, rep, q_hidden, p_hidden, w_up, w_down, pos_index, hard_index):
    pairs, length, features = q_hidden.shape[1:]
    hard = hard_index.shape[-1]
    hidden_units = w_up.shape[0]
    own_rows = hidden_units // (dp * rep)
    rows = -(-own_rows // ROW_TILE) * ROW_TILE
    depth = dp // 4
    members = 2 * rep
    strips = rows // ROW_TILE
    seqs = 2 * pairs
    count = seqs * length
    padded = -(-dp * seqs // LANES) * LANES
    chunk = members * 2 * rows

    def arrange(weight):
        blocks = weight.reshape(dp * rep, own_rows, features)
        if rows != own_rows:
            blocks = jnp.pad(blocks, ((0, 0), (0, rows - own_rows), (0, 0)))
        return blocks.reshape(depth, 2, members, rows, features)

    dma = pltpu.SemaphoreType.DMA
    hbm = pl.BlockSpec(memory_space=pl.ANY)
    fixed = pl.BlockSpec(memory_space=pltpu.HBM)
    vmem = pl.BlockSpec(memory_space=pltpu.VMEM)
    grad, loss = pl.pallas_call(
        functools.partial(kernel, dp, rep, pairs, length, hard),
        name="gradcache_step",
        out_shape=(
            pltpu.VMEM((rows, features), F32),
            pltpu.VMEM((1, 1), F32),
        ),
        in_specs=[hbm] * 4 + [fixed] * 2,
        out_specs=(vmem, vmem),
        scratch_shapes=[
            pltpu.VMEM((depth, members, 2, rows, features), BF16),
            pltpu.VMEM((depth, members, 2, rows, features), BF16),
            pltpu.VMEM((members, count, features), BF16),
            pltpu.VMEM((count, depth * chunk), BF16),
            pltpu.VMEM((depth, chunk, count), F32),
            pltpu.VMEM((count, features), F32),
            pltpu.VMEM((count, 1), F32),
            pltpu.VMEM((count, features), BF16),
            pltpu.VMEM((dp, seqs, features), BF16),
            pltpu.VMEM((dp, seqs, LANES), jnp.int32),
            pltpu.VMEM((padded, features), F32),
            pltpu.VMEM((padded, LANES), jnp.int32),
            pltpu.VMEM((depth, members, 2, rows, count), BF16),
            pltpu.VMEM((depth, members, 2, rows, count), BF16),
            pltpu.VMEM((2, ROW_TILE, features), F32),
            pltpu.VMEM((depth, rows, features), F32),
            pltpu.VMEM((depth, rows, features), BF16),
            pltpu.VMEM((depth, rows, features), BF16),
            pltpu.VMEM((depth, rows, features), BF16),
            pltpu.VMEM((depth, rows, features), BF16),
            pltpu.VMEM((rep, 1, LANES), F32),
            pltpu.SMEM((1, pairs), jnp.int32), pltpu.SMEM((pairs, hard), jnp.int32),
            dma((4,)), dma((2, depth)),
            dma((rep,)), dma((rep,)), dma((rep,)), dma((rep,)),
            dma((1,)), dma((1,)), dma((1,)), dma((1,)),
            dma((rep,)), dma((rep,)),
            dma((1,)), dma((depth, strips)), dma((1,)), dma((depth, strips)),
            dma((1,)), dma((1,)),
            pltpu.SemaphoreType.REGULAR, pltpu.SemaphoreType.REGULAR,
        ],
        compiler_params=pltpu.CompilerParams(
            collective_id=0, has_side_effects=True, vmem_limit_bytes=60 * 1024 * 1024
        ),
    )(
        q_hidden.reshape(pairs * length, features),
        p_hidden.reshape(pairs * length, features),
        arrange(w_up),
        arrange(w_down),
        pos_index.reshape(1, pairs),
        hard_index.reshape(pairs, hard),
    )
    return grad[:own_rows], loss.reshape(())


def solution(mesh):
    return jax.shard_map(
        functools.partial(shards, mesh.shape["dp"], mesh.shape["rep"]),
        mesh=mesh,
        in_specs=(
            P("rep", "dp", None, None),
            P("rep", "dp", None, None),
            P(),
            P(),
            P("rep", "dp"),
            P("rep", "dp", None),
        ),
        out_specs=(P(("dp", "rep"), None), P()),
        check_vma=False,
    )
```

```python
import functools
import math

import jax
import jax.numpy as jnp
from jax import lax
from jax.experimental import pallas as pl
from jax.experimental.pallas import tpu as pltpu
from jax.sharding import PartitionSpec as P

norm_eps = 1e-06
HARD_BOOST = 1.5
MESH = pl.DeviceIdType.MESH
LANES = 128
ROW_TILE = 16
LAGS = (6, 3)
F32 = jnp.float32
BF16 = jnp.bfloat16


def dot_nt(left, right):
    return lax.dot_general(
        left, right, (((1,), (1,)), ((), ())), preferred_element_type=F32
    )


def phi(values):
    return 0.5 * (1.0 + lax.erf(values * (1.0 / math.sqrt(2.0))))


def loop(count, body):
    if count <= 16:
        for step in range(count):
            body(step)
    else:
        lax.fori_loop(0, count, lambda step, carry: (body(step), carry)[1], 0)


def pipeline(tasks):
    cuts = sorted({edge - offset for _, first, last, offset in tasks for edge in (first, last)})
    for low, high in zip(cuts[:-1], cuts[1:]):
        active = [
            (body, offset) for body, first, last, offset in tasks
            if first <= low + offset and high + offset <= last
        ]

        def step_body(step, low=low, active=active):
            for body, offset in active:
                body(low + step + offset)

        loop(high - low, step_body)


def kernel(
    dp, pairs, length, hard,
    q_ref, p_ref, up_ref, down_ref, pos_ref, hard_ref,
    out_ref, loss_ref,
    up, down, tokens, hidden, normed, scales, slope, mixed, grads, slots, index_slots, every, index_rows,
    first_out, first_in, first_kept, second_out, second_in, second_kept, z_out, z_in, losses,
    pos_smem, hard_smem, t_sem, w_sem, d_send, d_recv, i_send, i_recv, e_send, e_recv,
    l_send, l_recv, first_send, first_recv, second_send, second_recv, z_send, z_recv,
):
    depth = dp // 4
    seqs = 2 * pairs
    count = seqs * length
    features = tokens.shape[-1]
    half = features // 2
    rows = up.shape[-2]
    block = 4 * rows
    chunk = 8 * rows
    strips = rows // ROW_TILE
    padded = every.shape[0]
    me = lax.axis_index("dp")
    my_rep = lax.axis_index("rep")
    other_rep = 1 - my_rep
    core = lax.rem(me, 2)
    side = lax.rem(me // 2, 2)
    layer = me // 4
    partner = me + 1 - 2 * core
    opposite = me + 2 - 4 * side

    def remote(src, dst, send, recv, device):
        return pltpu.make_async_remote_copy(
            src_ref=src, dst_ref=dst, send_sem=send, recv_sem=recv,
            device_id=device, device_id_type=MESH,
        )

    def ahead(step):
        return lax.rem(me + step, dp)

    half_count = pairs * length
    load_q = pltpu.make_async_copy(q_ref, tokens.at[core, pl.ds(0, half_count)], t_sem.at[0])
    load_p = pltpu.make_async_copy(p_ref, tokens.at[core, pl.ds(half_count, half_count)], t_sem.at[1])
    load_q.start()
    load_p.start()
    load_pos = pltpu.make_async_copy(pos_ref, pos_smem, t_sem.at[2])
    load_hard = pltpu.make_async_copy(hard_ref, hard_smem, t_sem.at[3])

    def load(which, step):
        ref, buffer = ((up_ref, up), (down_ref, down))[which]
        return pltpu.make_async_copy(ref.at[step], buffer.at[step], w_sem.at[which, step])

    loop(depth, lambda step: load(0, step).start())
    loop(depth, lambda step: load(1, step).start())
    load_pos.start()
    load_hard.start()

    barrier = pltpu.get_barrier_semaphore()

    def greet(step):
        pl.semaphore_signal(
            barrier, inc=1, device_id=(ahead(step + 1), my_rep), device_id_type=MESH
        )

    loop(dp - 1, greet)
    pl.semaphore_signal(barrier, inc=1, device_id=(me, other_rep), device_id_type=MESH)

    every[...] = jnp.zeros_like(every)
    index_rows[...] = jnp.full(index_rows.shape, -1, jnp.int32)

    load_q.wait()
    load_p.wait()
    own = tokens[core]

    def forward(step):
        load(0, step).wait()
        pre = dot_nt(own, up[step].reshape(chunk, features))
        columns = pl.ds(pl.multiple_of(step * chunk, chunk), chunk)
        hidden[:, columns] = (pre * phi(pre)).astype(BF16)

    loop(depth, forward)
    loop(depth, lambda step: load(1, step).wait())
    summed = own.astype(F32) + jnp.dot(
        hidden[...], down[...].reshape(depth * chunk, features), preferred_element_type=F32
    )

    means = []
    for seq in range(seqs):
        place = pl.ds(seq * length, length)
        part = summed[seq * length:(seq + 1) * length]
        centred = part - jnp.mean(part, -1, keepdims=True)
        scale = lax.rsqrt(jnp.mean(centred * centred, -1, keepdims=True) + norm_eps)
        unit = centred * scale
        normed[core, place, :] = unit.astype(BF16)
        scales[core, :, place] = jnp.broadcast_to(scale, (length, LANES)).T[0:8]
        means.append(jnp.mean(unit, 0, keepdims=True))
    slots[me] = jnp.concatenate(means, 0).astype(BF16)

    load_pos.wait()
    load_hard.wait()
    row_ids = lax.broadcasted_iota(jnp.int32, (seqs, LANES), 0)
    lane_ids = lax.broadcasted_iota(jnp.int32, (seqs, LANES), 1)
    message = jnp.full((seqs, LANES), -1, jnp.int32)
    for row in range(pairs):
        message = jnp.where((row_ids == row) & (lane_ids == 0), pos_smem[0, row], message)
        for pick in range(hard):
            message = jnp.where(
                (row_ids == row) & (lane_ids == 1 + pick), hard_smem[row, pick], message
            )
    index_slots[me] = message

    pl.semaphore_wait(barrier, dp)

    def embed_copy(step):
        return remote(
            slots.at[me], slots.at[me], e_send.at[0], e_recv.at[0],
            (ahead(step + 1), my_rep),
        )

    def index_copy(step):
        return remote(
            index_slots.at[me], index_slots.at[me], i_send.at[0], i_recv.at[0],
            (ahead(step + 1), my_rep),
        )

    loop(dp - 1, lambda step: embed_copy(step).start())
    loop(dp - 1, lambda step: index_copy(step).start())

    def twin_copy(which, slot):
        ref = (tokens, normed, scales)[which].at[slot]
        return remote(ref, ref, d_send.at[which], d_recv.at[which], (partner, my_rep))

    for which in range(3):
        twin_copy(which, core).start()

    def mix(step, slot):
        pre = dot_nt(up[step, :, core].reshape(block, features), tokens[slot])
        bell = jnp.exp(-0.5 * pre * pre) * (1.0 / math.sqrt(2.0 * math.pi))
        slope[slot, step] = (phi(pre) + pre * bell) * scales[slot][0:1]
        mixed[slot, step] = dot_nt(down[step, :, core].reshape(block, features), normed[slot])

    loop(depth, lambda step: mix(step, core))
    for which in range(3):
        twin_copy(which, 1 - core).wait_recv()
    loop(depth, lambda step: mix(step, 1 - core))

    def all_indices():
        landed = index_slots.at[pl.ds(0, dp - 1)]
        return remote(landed, landed, i_send.at[0], i_recv.at[0], (me, my_rep))

    def all_embeds():
        landed = slots.at[pl.ds(0, dp - 1)]
        return remote(landed, landed, e_send.at[0], e_recv.at[0], (me, my_rep))

    all_indices().wait_recv()
    all_embeds().wait_recv()
    for slot in range(dp):
        every[slot * seqs:(slot + 1) * seqs, :] = slots[slot].astype(F32)
        index_rows[slot * seqs:(slot + 1) * seqs, :] = index_slots[slot]

    embeds = every[...].astype(BF16)
    scores = dot_nt(embeds, embeds)
    row = lax.broadcasted_iota(jnp.int32, (padded, padded), 0)
    column = lax.broadcasted_iota(jnp.int32, (padded, padded), 1)
    row_place = lax.rem(row, seqs)
    column_place = lax.rem(column, seqs)
    valid = (
        (row < dp * seqs) & (row_place < pairs) & (column < dp * seqs) & (column_place >= pairs)
    )
    passage = (column // seqs) * pairs + column_place - pairs
    indices = index_rows[...]
    target = valid & (passage == indices[:, 0:1])
    is_hard = passage == indices[:, 1:2]
    for pick in range(1, hard):
        is_hard = is_hard | (passage == indices[:, 1 + pick:2 + pick])
    logits = scores + jnp.where(is_hard, HARD_BOOST, 0.0)
    row_max = jnp.max(jnp.where(valid, logits, -1e30), -1, keepdims=True)
    powers = jnp.where(valid, jnp.exp(jnp.where(valid, logits - row_max, 0.0)), 0.0)
    powers_sum = jnp.sum(powers, -1, keepdims=True)
    log_total = row_max + jnp.log(jnp.where(powers_sum > 0.0, powers_sum, 1.0))
    picked = jnp.sum(jnp.where(target, logits, 0.0), -1, keepdims=True)
    weights = jnp.where(
        valid,
        jnp.exp(jnp.where(valid, logits - log_total, 0.0)) - jnp.where(target, 1.0, 0.0),
        0.0,
    )
    both = weights + weights.T
    chip_seqs = 2 * seqs
    first_row = (me - core) * seqs
    chip_weights = jnp.concatenate(
        [
            jnp.sum(jnp.where(row == first_row + seq, both, 0.0), 0, keepdims=True)
            for seq in range(chip_seqs)
        ]
        + [jnp.zeros((-chip_seqs % 8, padded), F32)] * (1 if chip_seqs % 8 else 0),
        0,
    ).astype(BF16)
    d_chip = jnp.dot(chip_weights, embeds, preferred_element_type=F32) * (1.0 / length)
    d_low = (d_chip - jnp.mean(d_chip, -1, keepdims=True)).astype(BF16)
    aligned = [dot_nt(d_low, normed[slot]) * (1.0 / features) for slot in range(2)]
    row_one = lax.broadcasted_iota(jnp.int32, (padded, 1), 0)
    counted = (row_one < dp * seqs) & (lax.rem(row_one, seqs) < pairs)
    loss = jnp.sum(jnp.where(counted, log_total - picked, 0.0), 0, keepdims=True)
    losses[my_rep] = jnp.broadcast_to(loss, (1, LANES))

    def loss_copy(group):
        return remote(
            losses.at[group], losses.at[group], l_send.at[0], l_recv.at[0], (me, other_rep)
        )

    def strip(sub):
        return pl.ds(sub * ROW_TILE, ROW_TILE)

    def turn(step):
        own_turn = (step + 1) // depth
        upper = (2 * layer) // depth
        mirrored = upper * layer + (1 - upper) * (depth - 1 - layer)
        place = step + (step - mirrored + depth) // depth
        place = upper * place + (1 - upper) * (depth - 1 - place)
        return own_turn * layer + (1 - own_turn) * place

    def place_of(index):
        if strips == 1:
            return turn(index), 0
        return turn(index // strips), index % strips

    low, high = slice(0, half), slice(half, features)

    def backward(step):
        now = turn(step)
        spread = dot_nt(down[now, :, core].reshape(block, features), d_low)
        for slot in range(2):
            for seq in range(seqs):
                which = slot * seqs + seq
                place = slice(seq * length, (seq + 1) * length)
                grads[:, slot * count + seq * length:slot * count + (seq + 1) * length] = (
                    slope[slot, now, :, place]
                    * (
                        spread[:, which:which + 1]
                        - aligned[slot][which:which + 1, place] * mixed[slot, now, :, place]
                    )
                ).astype(BF16)
        total = jnp.dot(
            grads[...], tokens[...].reshape(2 * count, features), preferred_element_type=F32
        ).reshape(2, 2, rows, features)
        by_side = [total[0, :, :, high], total[1, :, :, high]]
        by_rep = [total[:, 0, :, low], total[:, 1, :, low]]
        mine = (my_rep == 0)
        first_out[now, 0] = jnp.where(mine, by_rep[1], by_rep[0]).astype(BF16)
        first_kept[now, 0] = jnp.where(mine, by_rep[0], by_rep[1])
        mine = (side == 0)
        first_out[now, 1] = jnp.where(mine, by_side[1], by_side[0]).astype(BF16)
        first_kept[now, 1] = jnp.where(mine, by_side[0], by_side[1])

    across = ((me, other_rep), (opposite, my_rep))

    def first_copy(now, sub, way):
        return remote(
            first_out.at[now, way, :, strip(sub)], first_in.at[now, way, :, strip(sub)],
            first_send.at[way], first_recv.at[now, sub, way], across[way],
        )

    def second_copy(now, sub, way):
        return remote(
            second_out.at[now, way, strip(sub)], second_in.at[now, way, strip(sub)],
            second_send.at[way], second_recv.at[now, sub, way], across[1 - way],
        )

    def z_copy(now, sub):
        return remote(
            z_out.at[now, strip(sub)], z_in.at[layer, strip(sub)],
            z_send.at[0], z_recv.at[0],
            (now * 4 + side * 2 + core, my_rep),
        )

    def send_first(index):
        now, sub = place_of(index)
        for way in range(2):
            first_copy(now, sub, way).start()

    def stage_two(index):
        now, sub = place_of(index)
        for way in range(2):
            stays = (side, my_rep)[way]
            first_copy(now, sub, way).wait_recv()
            second_out[now, way, strip(sub), :] = (
                first_kept[now, way, 1 - stays, strip(sub), :]
                + first_in[now, way, 1 - stays, strip(sub), :].astype(F32)
            ).astype(BF16)
            second_copy(now, sub, way).start()
            second_kept[now, way, strip(sub), :] = (
                first_kept[now, way, stays, strip(sub), :]
                + first_in[now, way, stays, strip(sub), :].astype(F32)
            )

    def stage_three(index, last):
        now, sub = place_of(index)
        for way in range(2):
            second_copy(now, sub, way).wait_recv()
            total = second_kept[now, way, strip(sub), :] + second_in[now, way, strip(sub), :].astype(F32)
            if last:
                out_ref[strip(sub), (low, high)[way]] = total
            else:
                z_out[now, strip(sub), (low, high)[way]] = total.astype(BF16)
        if not last:
            z_copy(now, sub).start()

    steps = depth * strips
    moved = steps - strips
    lag_one, lag_two = LAGS
    early = min(depth, -(-lag_one // strips))

    def backward_and_send(step):
        backward(step)
        for sub in range(strips):
            send_first(step * strips + sub)

    loop(early, backward_and_send)
    loss_copy(my_rep).start()
    loop(depth - early, lambda step: backward(step + early))
    sent = early * strips
    pipeline([
        (send_first, sent, steps, sent),
        (stage_two, 0, steps, 0),
        (lambda index: stage_three(index, False), 0, moved, -lag_two),
        (lambda index: stage_three(index, True), moved, steps, -lag_two),
    ])

    def all_layers():
        landed = z_in.at[pl.ds(0, depth - 1)]
        return remote(landed, landed, z_send.at[0], z_recv.at[0], (opposite, my_rep))

    all_layers().wait_recv()

    def collect(step):
        source = lax.rem(layer + depth - 1 - step, depth)
        out_ref[...] += z_in[source].astype(F32)

    loop(depth - 1, collect)

    loss_copy(other_rep).wait_recv()
    loss_ref[...] = (losses[0] + losses[1])[:, 0:1] * (1.0 / (dp * pairs * 2))

    all_indices().wait_send()
    all_embeds().wait_send()
    for which in range(3):
        twin_copy(which, core).wait_send()
    loss_copy(my_rep).wait_send()
    for way in range(2):
        sent_first = first_out.at[:, way]
        remote(sent_first, sent_first, first_send.at[way], first_recv.at[0, 0, way], across[way]).wait_send()
        sent_second = second_out.at[:, way]
        remote(sent_second, sent_second, second_send.at[way], second_recv.at[0, 0, way], across[1 - way]).wait_send()
    all_layers().wait_send()


def shards(dp, rep, q_hidden, p_hidden, w_up, w_down, pos_index, hard_index):
    assert rep == 2 and dp % 4 == 0
    pairs, length, features = q_hidden.shape[1:]
    hard = hard_index.shape[-1]
    hidden_units = w_up.shape[0]
    own_rows = hidden_units // (dp * rep)
    rows = -(-own_rows // ROW_TILE) * ROW_TILE
    depth = dp // 4
    strips = rows // ROW_TILE
    seqs = 2 * pairs
    count = seqs * length
    padded = -(-dp * seqs // LANES) * LANES
    chunk = 8 * rows
    half = features // 2

    def arrange(weight):
        blocks = weight.reshape(dp * rep, own_rows, features)
        if rows != own_rows:
            blocks = jnp.pad(blocks, ((0, 0), (0, rows - own_rows), (0, 0)))
        return blocks.reshape(depth, 2, 2, 2, rows, features)

    dma = pltpu.SemaphoreType.DMA
    hbm = pl.BlockSpec(memory_space=pl.ANY)
    fixed = pl.BlockSpec(memory_space=pltpu.HBM)
    vmem = pl.BlockSpec(memory_space=pltpu.VMEM)
    grad, loss = pl.pallas_call(
        functools.partial(kernel, dp, pairs, length, hard),
        name="gradcache_step",
        out_shape=(
            pltpu.VMEM((rows, features), F32),
            pltpu.VMEM((1, 1), F32),
        ),
        in_specs=[hbm] * 4 + [fixed] * 2,
        out_specs=(vmem, vmem),
        scratch_shapes=[
            pltpu.VMEM((depth, 2, 2, 2, rows, features), BF16),
            pltpu.VMEM((depth, 2, 2, 2, rows, features), BF16),
            pltpu.VMEM((2, count, features), BF16),
            pltpu.VMEM((count, depth * chunk), BF16),
            pltpu.VMEM((2, count, features), BF16),
            pltpu.VMEM((2, 8, count), F32),
            pltpu.VMEM((2, depth, 4 * rows, count), F32),
            pltpu.VMEM((2, depth, 4 * rows, count), F32),
            pltpu.VMEM((4 * rows, 2 * count), BF16),
            pltpu.VMEM((dp, seqs, features), BF16),
            pltpu.VMEM((dp, seqs, LANES), jnp.int32),
            pltpu.VMEM((padded, features), F32),
            pltpu.VMEM((padded, LANES), jnp.int32),
            pltpu.VMEM((depth, 2, 2, rows, half), BF16),
            pltpu.VMEM((depth, 2, 2, rows, half), BF16),
            pltpu.VMEM((depth, 2, 2, rows, half), F32),
            pltpu.VMEM((depth, 2, rows, half), BF16),
            pltpu.VMEM((depth, 2, rows, half), BF16),
            pltpu.VMEM((depth, 2, rows, half), F32),
            pltpu.VMEM((depth, rows, features), BF16),
            pltpu.VMEM((depth, rows, features), BF16),
            pltpu.VMEM((2, 1, LANES), F32),
            pltpu.SMEM((1, pairs), jnp.int32), pltpu.SMEM((pairs, hard), jnp.int32),
            dma((4,)), dma((2, depth)),
            dma((3,)), dma((3,)), dma((1,)), dma((1,)), dma((1,)), dma((1,)),
            dma((1,)), dma((1,)),
            dma((2,)), dma((depth, strips, 2)), dma((2,)), dma((depth, strips, 2)),
            dma((1,)), dma((1,)),
        ],
        compiler_params=pltpu.CompilerParams(
            collective_id=0, has_side_effects=True, vmem_limit_bytes=60 * 1024 * 1024
        ),
    )(
        q_hidden.reshape(pairs * length, features),
        p_hidden.reshape(pairs * length, features),
        arrange(w_up),
        arrange(w_down),
        pos_index.reshape(1, pairs),
        hard_index.reshape(pairs, hard),
    )
    return grad[:own_rows], loss.reshape(())


def solution(mesh):
    return jax.shard_map(
        functools.partial(shards, mesh.shape["dp"], mesh.shape["rep"]),
        mesh=mesh,
        in_specs=(
            P("rep", "dp", None, None),
            P("rep", "dp", None, None),
            P(),
            P(),
            P("rep", "dp"),
            P("rep", "dp", None),
        ),
        out_specs=(P(("dp", "rep"), None), P()),
        check_vma=False,
    )
```

```python
import functools
import math

import jax
import jax.numpy as jnp
from jax import lax
from jax.experimental import pallas as pl
from jax.experimental.pallas import tpu as pltpu
from jax.sharding import PartitionSpec as P

norm_eps = 1e-06
HARD_BOOST = 1.5
MESH = pl.DeviceIdType.MESH
LANES = 128
ROW_TILE = 16
LAGS = (6, 5)
F32 = jnp.float32
BF16 = jnp.bfloat16


def dot_nt(left, right):
    return lax.dot_general(
        left, right, (((1,), (1,)), ((), ())), preferred_element_type=F32
    )


def phi(values):
    return 0.5 * (1.0 + lax.erf(values * (1.0 / math.sqrt(2.0))))


def loop(count, body):
    if count <= 16:
        for step in range(count):
            body(step)
    else:
        lax.fori_loop(0, count, lambda step, carry: (body(step), carry)[1], 0)


def pipeline(tasks):
    cuts = sorted({edge - offset for _, first, last, offset in tasks for edge in (first, last)})
    for low, high in zip(cuts[:-1], cuts[1:]):
        active = [
            (body, offset) for body, first, last, offset in tasks
            if first <= low + offset and high + offset <= last
        ]

        def step_body(step, low=low, active=active):
            for body, offset in active:
                body(low + step + offset)

        loop(high - low, step_body)


def kernel(
    dp, pairs, length, hard,
    q_ref, p_ref, up_ref, down_ref, pos_ref, hard_ref,
    out_ref, loss_ref,
    up, down, tokens, hidden, normed, scales, slope, mixed, grads, slots, index_slots, every, index_rows,
    first_out, first_in, first_kept, second_out, second_in, second_kept, z_out, z_in, losses,
    pos_smem, hard_smem, t_sem, w_sem, d_send, d_recv, i_send, i_recv, e_send, e_recv,
    l_send, l_recv, first_send, first_recv, second_send, second_recv, z_send, z_recv,
):
    depth = dp // 4
    seqs = 2 * pairs
    count = seqs * length
    features = tokens.shape[-1]
    half = features // 2
    rows = up.shape[-2]
    block = 4 * rows
    chunk = 8 * rows
    strips = rows // ROW_TILE
    padded = every.shape[0]
    me = lax.axis_index("dp")
    my_rep = lax.axis_index("rep")
    other_rep = 1 - my_rep
    core = lax.rem(me, 2)
    side = lax.rem(me // 2, 2)
    layer = me // 4
    partner = me + 1 - 2 * core
    opposite = me + 2 - 4 * side

    def remote(src, dst, send, recv, device):
        return pltpu.make_async_remote_copy(
            src_ref=src, dst_ref=dst, send_sem=send, recv_sem=recv,
            device_id=device, device_id_type=MESH,
        )

    def ahead(step):
        return lax.rem(me + step, dp)

    half_count = pairs * length
    load_q = pltpu.make_async_copy(q_ref, tokens.at[core, pl.ds(0, half_count)], t_sem.at[0])
    load_p = pltpu.make_async_copy(p_ref, tokens.at[core, pl.ds(half_count, half_count)], t_sem.at[1])
    load_q.start()
    load_p.start()
    load_pos = pltpu.make_async_copy(pos_ref, pos_smem, t_sem.at[2])
    load_hard = pltpu.make_async_copy(hard_ref, hard_smem, t_sem.at[3])

    def load(which, step):
        ref, buffer = ((up_ref, up), (down_ref, down))[which]
        return pltpu.make_async_copy(ref.at[step], buffer.at[step], w_sem.at[which, step])

    loop(depth, lambda step: load(0, step).start())
    loop(depth, lambda step: load(1, step).start())
    load_pos.start()
    load_hard.start()

    barrier = pltpu.get_barrier_semaphore()

    def greet(step):
        pl.semaphore_signal(
            barrier, inc=1, device_id=(ahead(step + 1), my_rep), device_id_type=MESH
        )

    loop(dp - 1, greet)
    pl.semaphore_signal(barrier, inc=1, device_id=(me, other_rep), device_id_type=MESH)

    every[...] = jnp.zeros_like(every)
    index_rows[...] = jnp.full(index_rows.shape, -1, jnp.int32)

    load_q.wait()
    load_p.wait()
    own = tokens[core]

    def forward(step):
        pre = dot_nt(own, up[pl.ds(step * span, span)].reshape(span * chunk, features))
        columns = pl.ds(pl.multiple_of(step * span * chunk, span * chunk), span * chunk)
        hidden[:, columns] = (pre * phi(pre)).astype(BF16)

    span = 2 - depth % 2
    loop(depth, lambda step: load(0, step).wait())
    loop(depth // span, forward)
    loop(depth, lambda step: load(1, step).wait())
    summed = own.astype(F32) + jnp.dot(
        hidden[...], down[...].reshape(depth * chunk, features), preferred_element_type=F32
    )

    means = []
    for seq in range(seqs):
        place = pl.ds(seq * length, length)
        part = summed[seq * length:(seq + 1) * length]
        centred = part - jnp.mean(part, -1, keepdims=True)
        scale = lax.rsqrt(jnp.mean(centred * centred, -1, keepdims=True) + norm_eps)
        unit = centred * scale
        normed[core, place, :] = unit.astype(BF16)
        scales[core, :, place] = jnp.broadcast_to(scale, (length, LANES)).T[0:8]
        means.append(jnp.mean(unit, 0, keepdims=True))
    slots[me] = jnp.concatenate(means, 0).astype(BF16)

    load_pos.wait()
    load_hard.wait()
    row_ids = lax.broadcasted_iota(jnp.int32, (seqs, LANES), 0)
    lane_ids = lax.broadcasted_iota(jnp.int32, (seqs, LANES), 1)
    message = jnp.full((seqs, LANES), -1, jnp.int32)
    for row in range(pairs):
        message = jnp.where((row_ids == row) & (lane_ids == 0), pos_smem[0, row], message)
        for pick in range(hard):
            message = jnp.where(
                (row_ids == row) & (lane_ids == 1 + pick), hard_smem[row, pick], message
            )
    index_slots[me] = message

    pl.semaphore_wait(barrier, dp)

    def embed_copy(step):
        return remote(
            slots.at[me], slots.at[me], e_send.at[0], e_recv.at[0],
            (ahead(step + 1), my_rep),
        )

    def index_copy(step):
        return remote(
            index_slots.at[me], index_slots.at[me], i_send.at[0], i_recv.at[0],
            (ahead(step + 1), my_rep),
        )

    loop(dp - 1, lambda step: embed_copy(step).start())
    loop(dp - 1, lambda step: index_copy(step).start())

    def twin_copy(which, slot):
        ref = (tokens, normed, scales)[which].at[slot]
        return remote(ref, ref, d_send.at[which], d_recv.at[which], (partner, my_rep))

    for which in range(3):
        twin_copy(which, core).start()

    def mix(step, slot):
        pre = dot_nt(up[step, :, core].reshape(block, features), tokens[slot])
        bell = jnp.exp(-0.5 * pre * pre) * (1.0 / math.sqrt(2.0 * math.pi))
        slope[slot, step] = (phi(pre) + pre * bell) * scales[slot][0:1]
        mixed[slot, step] = dot_nt(down[step, :, core].reshape(block, features), normed[slot])

    loop(depth, lambda step: mix(step, core))
    for which in range(3):
        twin_copy(which, 1 - core).wait_recv()
    loop(depth, lambda step: mix(step, 1 - core))

    def all_indices():
        landed = index_slots.at[pl.ds(0, dp - 1)]
        return remote(landed, landed, i_send.at[0], i_recv.at[0], (me, my_rep))

    def all_embeds():
        landed = slots.at[pl.ds(0, dp - 1)]
        return remote(landed, landed, e_send.at[0], e_recv.at[0], (me, my_rep))

    all_indices().wait_recv()
    all_embeds().wait_recv()
    for slot in range(dp):
        every[slot * seqs:(slot + 1) * seqs, :] = slots[slot].astype(F32)
        index_rows[slot * seqs:(slot + 1) * seqs, :] = index_slots[slot]

    embeds = every[...].astype(BF16)
    scores = dot_nt(embeds, embeds)
    row = lax.broadcasted_iota(jnp.int32, (padded, padded), 0)
    column = lax.broadcasted_iota(jnp.int32, (padded, padded), 1)
    row_place = lax.rem(row, seqs)
    column_place = lax.rem(column, seqs)
    valid = (
        (row < dp * seqs) & (row_place < pairs) & (column < dp * seqs) & (column_place >= pairs)
    )
    passage = (column // seqs) * pairs + column_place - pairs
    indices = index_rows[...]
    target = valid & (passage == indices[:, 0:1])
    is_hard = passage == indices[:, 1:2]
    for pick in range(1, hard):
        is_hard = is_hard | (passage == indices[:, 1 + pick:2 + pick])
    logits = scores + jnp.where(is_hard, HARD_BOOST, 0.0)
    row_max = jnp.max(jnp.where(valid, logits, -1e30), -1, keepdims=True)
    powers = jnp.where(valid, jnp.exp(jnp.where(valid, logits - row_max, 0.0)), 0.0)
    powers_sum = jnp.sum(powers, -1, keepdims=True)
    log_total = row_max + jnp.log(jnp.where(powers_sum > 0.0, powers_sum, 1.0))
    picked = jnp.sum(jnp.where(target, logits, 0.0), -1, keepdims=True)
    weights = jnp.where(
        valid,
        jnp.exp(jnp.where(valid, logits - log_total, 0.0)) - jnp.where(target, 1.0, 0.0),
        0.0,
    )
    both = weights + weights.T
    chip_seqs = 2 * seqs
    first_row = (me - core) * seqs
    chip_weights = jnp.concatenate(
        [
            jnp.sum(jnp.where(row == first_row + seq, both, 0.0), 0, keepdims=True)
            for seq in range(chip_seqs)
        ]
        + [jnp.zeros((-chip_seqs % 8, padded), F32)] * (1 if chip_seqs % 8 else 0),
        0,
    ).astype(BF16)
    d_chip = jnp.dot(chip_weights, embeds, preferred_element_type=F32) * (1.0 / length)
    d_low = (d_chip - jnp.mean(d_chip, -1, keepdims=True)).astype(BF16)
    aligned = [dot_nt(d_low, normed[slot]) * (1.0 / features) for slot in range(2)]
    row_one = lax.broadcasted_iota(jnp.int32, (padded, 1), 0)
    counted = (row_one < dp * seqs) & (lax.rem(row_one, seqs) < pairs)
    loss = jnp.sum(jnp.where(counted, log_total - picked, 0.0), 0, keepdims=True)
    losses[my_rep] = jnp.broadcast_to(loss, (1, LANES))

    def loss_copy(group):
        return remote(
            losses.at[group], losses.at[group], l_send.at[0], l_recv.at[0], (me, other_rep)
        )

    def strip(sub):
        return pl.ds(sub * ROW_TILE, ROW_TILE)

    def turn(step):
        own_turn = (step + 1) // depth
        upper = (2 * layer) // depth
        mirrored = upper * layer + (1 - upper) * (depth - 1 - layer)
        place = step + (step - mirrored + depth) // depth
        place = upper * place + (1 - upper) * (depth - 1 - place)
        return own_turn * layer + (1 - own_turn) * place

    def place_of(index):
        if strips == 1:
            return turn(index), 0
        return turn(index // strips), index % strips

    low, high = slice(0, half), slice(half, features)

    def backward(step):
        now = turn(step)
        spread = dot_nt(down[now, :, core].reshape(block, features), d_low)
        for slot in range(2):
            for seq in range(seqs):
                which = slot * seqs + seq
                place = slice(seq * length, (seq + 1) * length)
                grads[:, slot * count + seq * length:slot * count + (seq + 1) * length] = (
                    slope[slot, now, :, place]
                    * (
                        spread[:, which:which + 1]
                        - aligned[slot][which:which + 1, place] * mixed[slot, now, :, place]
                    )
                ).astype(BF16)
        total = jnp.dot(
            grads[...], tokens[...].reshape(2 * count, features), preferred_element_type=F32
        ).reshape(2, 2, rows, features)
        by_side = [total[0, :, :, high], total[1, :, :, high]]
        by_rep = [total[:, 0, :, low], total[:, 1, :, low]]
        mine = (my_rep == 0)
        first_out[now, 0] = jnp.where(mine, by_rep[1], by_rep[0]).astype(BF16)
        first_kept[now, 0] = jnp.where(mine, by_rep[0], by_rep[1])
        mine = (side == 0)
        first_out[now, 1] = jnp.where(mine, by_side[1], by_side[0]).astype(BF16)
        first_kept[now, 1] = jnp.where(mine, by_side[0], by_side[1])

    across = ((me, other_rep), (opposite, my_rep))

    def first_copy(now, sub, way):
        return remote(
            first_out.at[now, way, :, strip(sub)], first_in.at[now, way, :, strip(sub)],
            first_send.at[way], first_recv.at[now, sub, way], across[way],
        )

    def second_copy(now, sub, way):
        return remote(
            second_out.at[now, way, strip(sub)], second_in.at[now, way, strip(sub)],
            second_send.at[way], second_recv.at[now, sub, way], across[1 - way],
        )

    def z_copy(now, sub):
        return remote(
            z_out.at[now, strip(sub)], z_in.at[layer, strip(sub)],
            z_send.at[0], z_recv.at[0],
            (now * 4 + side * 2 + core, my_rep),
        )

    def send_first(index):
        now, sub = place_of(index)
        for way in range(2):
            first_copy(now, sub, way).start()

    def stage_two(index):
        now, sub = place_of(index)
        for way in range(2):
            stays = (side, my_rep)[way]
            first_copy(now, sub, way).wait_recv()
            second_out[now, way, strip(sub), :] = (
                first_kept[now, way, 1 - stays, strip(sub), :]
                + first_in[now, way, 1 - stays, strip(sub), :].astype(F32)
            ).astype(BF16)
            second_copy(now, sub, way).start()
            second_kept[now, way, strip(sub), :] = (
                first_kept[now, way, stays, strip(sub), :]
                + first_in[now, way, stays, strip(sub), :].astype(F32)
            )

    def stage_three(index, last):
        now, sub = place_of(index)
        for way in range(2):
            second_copy(now, sub, way).wait_recv()
            total = second_kept[now, way, strip(sub), :] + second_in[now, way, strip(sub), :].astype(F32)
            if last:
                out_ref[strip(sub), (low, high)[way]] = total
            else:
                z_out[now, strip(sub), (low, high)[way]] = total.astype(BF16)
        if not last:
            z_copy(now, sub).start()

    steps = depth * strips
    moved = steps - strips
    lag_one, lag_two = LAGS
    early = min(depth, -(-lag_one // strips))

    def backward_and_send(step):
        backward(step)
        for sub in range(strips):
            send_first(step * strips + sub)

    loop(early, backward_and_send)
    loss_copy(my_rep).start()
    loop(depth - early, lambda step: backward(step + early))
    sent = early * strips
    pipeline([
        (send_first, sent, steps, sent),
        (stage_two, 0, steps, 0),
        (lambda index: stage_three(index, False), 0, moved, -lag_two),
        (lambda index: stage_three(index, True), moved, steps, -lag_two),
    ])

    def all_layers():
        landed = z_in.at[pl.ds(0, depth - 1)]
        return remote(landed, landed, z_send.at[0], z_recv.at[0], (opposite, my_rep))

    all_layers().wait_recv()

    def collect(step):
        source = lax.rem(layer + depth - 1 - step, depth)
        out_ref[...] += z_in[source].astype(F32)

    loop(depth - 1, collect)

    loss_copy(other_rep).wait_recv()
    loss_ref[...] = (losses[0] + losses[1])[:, 0:1] * (1.0 / (dp * pairs * 2))

    all_indices().wait_send()
    all_embeds().wait_send()
    for which in range(3):
        twin_copy(which, core).wait_send()
    loss_copy(my_rep).wait_send()
    for way in range(2):
        sent_first = first_out.at[:, way]
        remote(sent_first, sent_first, first_send.at[way], first_recv.at[0, 0, way], across[way]).wait_send()
        sent_second = second_out.at[:, way]
        remote(sent_second, sent_second, second_send.at[way], second_recv.at[0, 0, way], across[1 - way]).wait_send()
    all_layers().wait_send()


def shards(dp, rep, q_hidden, p_hidden, w_up, w_down, pos_index, hard_index):
    assert rep == 2 and dp % 4 == 0
    pairs, length, features = q_hidden.shape[1:]
    hard = hard_index.shape[-1]
    hidden_units = w_up.shape[0]
    own_rows = hidden_units // (dp * rep)
    rows = -(-own_rows // ROW_TILE) * ROW_TILE
    depth = dp // 4
    strips = rows // ROW_TILE
    seqs = 2 * pairs
    count = seqs * length
    padded = -(-dp * seqs // LANES) * LANES
    chunk = 8 * rows
    half = features // 2

    def arrange(weight):
        blocks = weight.reshape(dp * rep, own_rows, features)
        if rows != own_rows:
            blocks = jnp.pad(blocks, ((0, 0), (0, rows - own_rows), (0, 0)))
        return blocks.reshape(depth, 2, 2, 2, rows, features)

    dma = pltpu.SemaphoreType.DMA
    hbm = pl.BlockSpec(memory_space=pl.ANY)
    fixed = pl.BlockSpec(memory_space=pltpu.HBM)
    vmem = pl.BlockSpec(memory_space=pltpu.VMEM)
    grad, loss = pl.pallas_call(
        functools.partial(kernel, dp, pairs, length, hard),
        name="gradcache_step",
        out_shape=(
            pltpu.VMEM((rows, features), F32),
            pltpu.VMEM((1, 1), F32),
        ),
        in_specs=[hbm] * 4 + [fixed] * 2,
        out_specs=(vmem, vmem),
        scratch_shapes=[
            pltpu.VMEM((depth, 2, 2, 2, rows, features), BF16),
            pltpu.VMEM((depth, 2, 2, 2, rows, features), BF16),
            pltpu.VMEM((2, count, features), BF16),
            pltpu.VMEM((count, depth * chunk), BF16),
            pltpu.VMEM((2, count, features), BF16),
            pltpu.VMEM((2, 8, count), F32),
            pltpu.VMEM((2, depth, 4 * rows, count), F32),
            pltpu.VMEM((2, depth, 4 * rows, count), F32),
            pltpu.VMEM((4 * rows, 2 * count), BF16),
            pltpu.VMEM((dp, seqs, features), BF16),
            pltpu.VMEM((dp, seqs, LANES), jnp.int32),
            pltpu.VMEM((padded, features), F32),
            pltpu.VMEM((padded, LANES), jnp.int32),
            pltpu.VMEM((depth, 2, 2, rows, half), BF16),
            pltpu.VMEM((depth, 2, 2, rows, half), BF16),
            pltpu.VMEM((depth, 2, 2, rows, half), F32),
            pltpu.VMEM((depth, 2, rows, half), BF16),
            pltpu.VMEM((depth, 2, rows, half), BF16),
            pltpu.VMEM((depth, 2, rows, half), F32),
            pltpu.VMEM((depth, rows, features), BF16),
            pltpu.VMEM((depth, rows, features), BF16),
            pltpu.VMEM((2, 1, LANES), F32),
            pltpu.SMEM((1, pairs), jnp.int32), pltpu.SMEM((pairs, hard), jnp.int32),
            dma((4,)), dma((2, depth)),
            dma((3,)), dma((3,)), dma((1,)), dma((1,)), dma((1,)), dma((1,)),
            dma((1,)), dma((1,)),
            dma((2,)), dma((depth, strips, 2)), dma((2,)), dma((depth, strips, 2)),
            dma((1,)), dma((1,)),
        ],
        compiler_params=pltpu.CompilerParams(
            collective_id=0, has_side_effects=True, vmem_limit_bytes=60 * 1024 * 1024
        ),
    )(
        q_hidden.reshape(pairs * length, features),
        p_hidden.reshape(pairs * length, features),
        arrange(w_up),
        arrange(w_down),
        pos_index.reshape(1, pairs),
        hard_index.reshape(pairs, hard),
    )
    return grad[:own_rows], loss.reshape(())


def solution(mesh):
    return jax.shard_map(
        functools.partial(shards, mesh.shape["dp"], mesh.shape["rep"]),
        mesh=mesh,
        in_specs=(
            P("rep", "dp", None, None),
            P("rep", "dp", None, None),
            P(),
            P(),
            P("rep", "dp"),
            P("rep", "dp", None),
        ),
        out_specs=(P(("dp", "rep"), None), P()),
        check_vma=False,
    )
```

```python
import functools
import math

import jax
import jax.numpy as jnp
from jax import lax
from jax.experimental import pallas as pl
from jax.experimental.pallas import tpu as pltpu
from jax.sharding import PartitionSpec as P

norm_eps = 1e-06
HARD_BOOST = 1.5
MESH = pl.DeviceIdType.MESH
LANES = 128
ROW_TILE = 16
LAGS = (6, 5)
F32 = jnp.float32
BF16 = jnp.bfloat16


def dot_nt(left, right):
    return lax.dot_general(
        left, right, (((1,), (1,)), ((), ())), preferred_element_type=F32
    )


def phi(values):
    return 0.5 * (1.0 + lax.erf(values * (1.0 / math.sqrt(2.0))))


def loop(count, body):
    if count <= 16:
        for step in range(count):
            body(step)
    else:
        lax.fori_loop(0, count, lambda step, carry: (body(step), carry)[1], 0)


def pipeline(tasks):
    cuts = sorted({edge - offset for _, first, last, offset in tasks for edge in (first, last)})
    for low, high in zip(cuts[:-1], cuts[1:]):
        active = [
            (body, offset) for body, first, last, offset in tasks
            if first <= low + offset and high + offset <= last
        ]

        def step_body(step, low=low, active=active):
            for body, offset in active:
                body(low + step + offset)

        loop(high - low, step_body)


def kernel(
    dp, pairs, length, hard,
    q_ref, p_ref, up_ref, down_ref, pos_ref, hard_ref,
    out_ref, loss_ref,
    up, down, tokens, hidden, normed, scales, slope, mixed, grads, slots, index_slots, every, index_rows,
    first_out, first_in, first_kept, second_out, second_in, second_kept, z_out, z_in, losses,
    pos_smem, hard_smem, t_sem, w_sem, d_send, d_recv, i_send, i_recv, e_send, e_recv,
    l_send, l_recv, first_send, first_recv, second_send, second_recv, z_send, z_recv,
):
    depth = dp // 4
    seqs = 2 * pairs
    count = seqs * length
    features = tokens.shape[-1]
    half = features // 2
    rows = up.shape[-2]
    block = 4 * rows
    chunk = 8 * rows
    strips = rows // ROW_TILE
    padded = every.shape[0]
    me = lax.axis_index("dp")
    my_rep = lax.axis_index("rep")
    other_rep = 1 - my_rep
    core = lax.rem(me, 2)
    side = lax.rem(me // 2, 2)
    layer = me // 4
    partner = me + 1 - 2 * core
    opposite = me + 2 - 4 * side

    def remote(src, dst, send, recv, device):
        return pltpu.make_async_remote_copy(
            src_ref=src, dst_ref=dst, send_sem=send, recv_sem=recv,
            device_id=device, device_id_type=MESH,
        )

    def ahead(step):
        return lax.rem(me + step, dp)

    half_count = pairs * length
    load_q = pltpu.make_async_copy(q_ref, tokens.at[core, pl.ds(0, half_count)], t_sem.at[0])
    load_p = pltpu.make_async_copy(p_ref, tokens.at[core, pl.ds(half_count, half_count)], t_sem.at[1])
    load_q.start()
    load_p.start()
    load_pos = pltpu.make_async_copy(pos_ref, pos_smem, t_sem.at[2])
    load_hard = pltpu.make_async_copy(hard_ref, hard_smem, t_sem.at[3])

    def load(which, step):
        ref, buffer = ((up_ref, up), (down_ref, down))[which]
        return pltpu.make_async_copy(ref.at[step], buffer.at[step], w_sem.at[which, step])

    loop(depth, lambda step: load(0, step).start())
    loop(depth, lambda step: load(1, step).start())
    load_pos.start()
    load_hard.start()

    barrier = pltpu.get_barrier_semaphore()

    def greet(step):
        pl.semaphore_signal(
            barrier, inc=1, device_id=(ahead(step + 1), my_rep), device_id_type=MESH
        )

    loop(dp - 1, greet)
    pl.semaphore_signal(barrier, inc=1, device_id=(me, other_rep), device_id_type=MESH)

    every[...] = jnp.zeros_like(every)
    index_rows[...] = jnp.full(index_rows.shape, -1, jnp.int32)

    load_q.wait()
    load_p.wait()
    own = tokens[core]

    def forward(step):
        pre = dot_nt(own, up[pl.ds(step * span, span)].reshape(span * chunk, features))
        columns = pl.ds(pl.multiple_of(step * span * chunk, span * chunk), span * chunk)
        hidden[:, columns] = (pre * phi(pre)).astype(BF16)

    span = 2 - depth % 2
    loop(depth, lambda step: load(0, step).wait())
    loop(depth // span, forward)
    loop(depth, lambda step: load(1, step).wait())
    summed = own.astype(F32) + jnp.dot(
        hidden[...], down[...].reshape(depth * chunk, features), preferred_element_type=F32
    )

    means = []
    for seq in range(seqs):
        place = pl.ds(seq * length, length)
        part = summed[seq * length:(seq + 1) * length]
        centred = part - jnp.mean(part, -1, keepdims=True)
        scale = lax.rsqrt(jnp.mean(centred * centred, -1, keepdims=True) + norm_eps)
        unit = centred * scale
        normed[core, place, :] = unit.astype(BF16)
        scales[core, :, place] = jnp.broadcast_to(scale, (length, LANES)).T[0:8]
        means.append(jnp.mean(unit, 0, keepdims=True))
    slots[me] = jnp.concatenate(means, 0).astype(BF16)

    load_pos.wait()
    load_hard.wait()
    row_ids = lax.broadcasted_iota(jnp.int32, (seqs, LANES), 0)
    lane_ids = lax.broadcasted_iota(jnp.int32, (seqs, LANES), 1)
    message = jnp.full((seqs, LANES), -1, jnp.int32)
    for row in range(pairs):
        message = jnp.where((row_ids == row) & (lane_ids == 0), pos_smem[0, row], message)
        for pick in range(hard):
            message = jnp.where(
                (row_ids == row) & (lane_ids == 1 + pick), hard_smem[row, pick], message
            )
    index_slots[me] = message

    pl.semaphore_wait(barrier, dp)

    def embed_copy(step):
        return remote(
            slots.at[me], slots.at[me], e_send.at[0], e_recv.at[0],
            (ahead(step + 1), my_rep),
        )

    def index_copy(step):
        return remote(
            index_slots.at[me], index_slots.at[me], i_send.at[0], i_recv.at[0],
            (ahead(step + 1), my_rep),
        )

    loop(dp - 1, lambda step: embed_copy(step).start())
    loop(dp - 1, lambda step: index_copy(step).start())

    def twin_copy(which, slot):
        ref = (tokens, normed, scales)[which].at[slot]
        return remote(ref, ref, d_send.at[which], d_recv.at[which], (partner, my_rep))

    for which in range(3):
        twin_copy(which, core).start()

    def mix(step, slot):
        pre = dot_nt(up[step, :, core].reshape(block, features), tokens[slot])
        bell = jnp.exp(-0.5 * pre * pre) * (1.0 / math.sqrt(2.0 * math.pi))
        slope[slot, step] = (phi(pre) + pre * bell) * scales[slot][0:1]
        mixed[slot, step] = dot_nt(down[step, :, core].reshape(block, features), normed[slot])

    loop(depth, lambda step: mix(step, core))
    for which in range(3):
        twin_copy(which, 1 - core).wait_recv()
    loop(depth, lambda step: mix(step, 1 - core))

    def all_indices():
        landed = index_slots.at[pl.ds(0, dp - 1)]
        return remote(landed, landed, i_send.at[0], i_recv.at[0], (me, my_rep))

    def all_embeds():
        landed = slots.at[pl.ds(0, dp - 1)]
        return remote(landed, landed, e_send.at[0], e_recv.at[0], (me, my_rep))

    all_indices().wait_recv()
    all_embeds().wait_recv()
    for slot in range(dp):
        every[slot * seqs:(slot + 1) * seqs, :] = slots[slot].astype(F32)
        index_rows[slot * seqs:(slot + 1) * seqs, :] = index_slots[slot]

    embeds = every[...].astype(BF16)
    scores = dot_nt(embeds, embeds)
    row = lax.broadcasted_iota(jnp.int32, (padded, padded), 0)
    column = lax.broadcasted_iota(jnp.int32, (padded, padded), 1)
    row_place = lax.rem(row, seqs)
    column_place = lax.rem(column, seqs)
    valid = (
        (row < dp * seqs) & (row_place < pairs) & (column < dp * seqs) & (column_place >= pairs)
    )
    passage = (column // seqs) * pairs + column_place - pairs
    indices = index_rows[...]
    target = valid & (passage == indices[:, 0:1])
    is_hard = passage == indices[:, 1:2]
    for pick in range(1, hard):
        is_hard = is_hard | (passage == indices[:, 1 + pick:2 + pick])
    logits = scores + jnp.where(is_hard, HARD_BOOST, 0.0)
    row_max = jnp.max(jnp.where(valid, logits, -1e30), -1, keepdims=True)
    powers = jnp.where(valid, jnp.exp(jnp.where(valid, logits - row_max, 0.0)), 0.0)
    powers_sum = jnp.sum(powers, -1, keepdims=True)
    log_total = row_max + jnp.log(jnp.where(powers_sum > 0.0, powers_sum, 1.0))
    picked = jnp.sum(jnp.where(target, logits, 0.0), -1, keepdims=True)
    weights = jnp.where(
        valid,
        jnp.exp(jnp.where(valid, logits - log_total, 0.0)) - jnp.where(target, 1.0, 0.0),
        0.0,
    )
    both = weights + weights.T
    chip_seqs = 2 * seqs
    first_row = (me - core) * seqs
    chip_weights = jnp.concatenate(
        [
            jnp.sum(jnp.where(row == first_row + seq, both, 0.0), 0, keepdims=True)
            for seq in range(chip_seqs)
        ]
        + [jnp.zeros((-chip_seqs % 8, padded), F32)] * (1 if chip_seqs % 8 else 0),
        0,
    ).astype(BF16)
    d_chip = jnp.dot(chip_weights, embeds, preferred_element_type=F32) * (1.0 / length)
    d_low = (d_chip - jnp.mean(d_chip, -1, keepdims=True)).astype(BF16)
    aligned = [dot_nt(d_low, normed[slot]) * (1.0 / features) for slot in range(2)]
    row_one = lax.broadcasted_iota(jnp.int32, (padded, 1), 0)
    counted = (row_one < dp * seqs) & (lax.rem(row_one, seqs) < pairs)
    loss = jnp.sum(jnp.where(counted, log_total - picked, 0.0), 0, keepdims=True)
    losses[my_rep] = jnp.broadcast_to(loss, (1, LANES))

    def loss_copy(group):
        return remote(
            losses.at[group], losses.at[group], l_send.at[0], l_recv.at[0], (me, other_rep)
        )

    def strip(sub):
        return pl.ds(sub * ROW_TILE, ROW_TILE)

    def turn(step):
        short = jnp.minimum(layer, depth - 1 - layer)
        ahead_first = jnp.where(2 * layer < depth, 1, -1)
        lone = depth - 1 - 2 * short
        late = jnp.maximum(step - lone, 0)
        return jnp.where(
            step < lone,
            layer + ahead_first * (depth - 1 - short - step),
            layer + ahead_first * (short - late // 2) * (2 * lax.rem(late, 2) - 1),
        )

    def place_of(index):
        if strips == 1:
            return turn(index), 0
        return turn(index // strips), index % strips

    low, high = slice(0, half), slice(half, features)

    def backward(step):
        now = turn(step)
        spread = dot_nt(down[now, :, core].reshape(block, features), d_low)
        for slot in range(2):
            for seq in range(seqs):
                which = slot * seqs + seq
                place = slice(seq * length, (seq + 1) * length)
                grads[:, slot * count + seq * length:slot * count + (seq + 1) * length] = (
                    slope[slot, now, :, place]
                    * (
                        spread[:, which:which + 1]
                        - aligned[slot][which:which + 1, place] * mixed[slot, now, :, place]
                    )
                ).astype(BF16)
        total = jnp.dot(
            grads[...], tokens[...].reshape(2 * count, features), preferred_element_type=F32
        ).reshape(2, 2, rows, features)
        by_side = [total[0, :, :, high], total[1, :, :, high]]
        by_rep = [total[:, 0, :, low], total[:, 1, :, low]]
        mine = (my_rep == 0)
        first_out[now, 0] = jnp.where(mine, by_rep[1], by_rep[0]).astype(BF16)
        first_kept[now, 0] = jnp.where(mine, by_rep[0], by_rep[1])
        mine = (side == 0)
        first_out[now, 1] = jnp.where(mine, by_side[1], by_side[0]).astype(BF16)
        first_kept[now, 1] = jnp.where(mine, by_side[0], by_side[1])

    across = ((me, other_rep), (opposite, my_rep))

    def first_copy(now, sub, way):
        return remote(
            first_out.at[now, way, :, strip(sub)], first_in.at[now, way, :, strip(sub)],
            first_send.at[way], first_recv.at[now, sub, way], across[way],
        )

    def second_copy(now, sub, way):
        return remote(
            second_out.at[now, way, strip(sub)], second_in.at[now, way, strip(sub)],
            second_send.at[way], second_recv.at[now, sub, way], across[1 - way],
        )

    def z_copy(now, sub):
        return remote(
            z_out.at[now, strip(sub)], z_in.at[layer, strip(sub)],
            z_send.at[0], z_recv.at[0],
            (now * 4 + side * 2 + core, my_rep),
        )

    def send_first(index):
        now, sub = place_of(index)
        for way in range(2):
            first_copy(now, sub, way).start()

    def stage_two(index):
        now, sub = place_of(index)
        for way in range(2):
            stays = (side, my_rep)[way]
            first_copy(now, sub, way).wait_recv()
            second_out[now, way, strip(sub), :] = (
                first_kept[now, way, 1 - stays, strip(sub), :]
                + first_in[now, way, 1 - stays, strip(sub), :].astype(F32)
            ).astype(BF16)
            second_copy(now, sub, way).start()
            second_kept[now, way, strip(sub), :] = (
                first_kept[now, way, stays, strip(sub), :]
                + first_in[now, way, stays, strip(sub), :].astype(F32)
            )

    def stage_three(index, last):
        now, sub = place_of(index)
        for way in range(2):
            second_copy(now, sub, way).wait_recv()
            total = second_kept[now, way, strip(sub), :] + second_in[now, way, strip(sub), :].astype(F32)
            if last:
                out_ref[strip(sub), (low, high)[way]] = total
            else:
                z_out[now, strip(sub), (low, high)[way]] = total.astype(BF16)
        if not last:
            z_copy(now, sub).start()

    steps = depth * strips
    moved = steps - strips
    lag_one, lag_two = LAGS
    early = min(depth, lag_one // strips)
    sent = min(steps, lag_one)

    def backward_and_send(step):
        backward(step)
        for sub in range(strips):
            send_first(step * strips + sub)

    loop(early, backward_and_send)
    loss_copy(my_rep).start()
    loop(depth - early, lambda step: backward(step + early))
    loop(sent - early * strips, lambda step: send_first(early * strips + step))
    pipeline([
        (send_first, sent, steps, sent),
        (stage_two, 0, steps, 0),
        (lambda index: stage_three(index, False), 0, moved, -lag_two),
        (lambda index: stage_three(index, True), moved, steps, -lag_two),
    ])

    def all_layers():
        landed = z_in.at[pl.ds(0, depth - 1)]
        return remote(landed, landed, z_send.at[0], z_recv.at[0], (opposite, my_rep))

    loss_copy(other_rep).wait_recv()
    loss_ref[0, 0] = (losses[0] + losses[1])[0, 0] * (1.0 / (dp * pairs * 2))
    all_layers().wait_recv()

    def collect(step):
        source = lax.rem(layer + depth - 1 - step, depth)
        out_ref[...] += z_in[source].astype(F32)

    loop(depth - 1, collect)

    all_indices().wait_send()
    all_embeds().wait_send()
    for which in range(3):
        twin_copy(which, core).wait_send()
    loss_copy(my_rep).wait_send()
    for way in range(2):
        sent_first = first_out.at[:, way]
        remote(sent_first, sent_first, first_send.at[way], first_recv.at[0, 0, way], across[way]).wait_send()
        sent_second = second_out.at[:, way]
        remote(sent_second, sent_second, second_send.at[way], second_recv.at[0, 0, way], across[1 - way]).wait_send()
    all_layers().wait_send()


def shards(dp, rep, q_hidden, p_hidden, w_up, w_down, pos_index, hard_index):
    assert rep == 2 and dp % 4 == 0
    pairs, length, features = q_hidden.shape[1:]
    hard = hard_index.shape[-1]
    hidden_units = w_up.shape[0]
    own_rows = hidden_units // (dp * rep)
    rows = -(-own_rows // ROW_TILE) * ROW_TILE
    depth = dp // 4
    strips = rows // ROW_TILE
    seqs = 2 * pairs
    count = seqs * length
    padded = -(-dp * seqs // LANES) * LANES
    chunk = 8 * rows
    half = features // 2

    def arrange(weight):
        blocks = weight.reshape(dp * rep, own_rows, features)
        if rows != own_rows:
            blocks = jnp.pad(blocks, ((0, 0), (0, rows - own_rows), (0, 0)))
        return blocks.reshape(depth, 2, 2, 2, rows, features)

    dma = pltpu.SemaphoreType.DMA
    hbm = pl.BlockSpec(memory_space=pl.ANY)
    fixed = pl.BlockSpec(memory_space=pltpu.HBM)
    vmem = pl.BlockSpec(memory_space=pltpu.VMEM)
    grad, loss = pl.pallas_call(
        functools.partial(kernel, dp, pairs, length, hard),
        name="gradcache_step",
        out_shape=(
            pltpu.VMEM((rows, features), F32),
            pltpu.SMEM((1, 1), F32),
        ),
        in_specs=[hbm] * 4 + [fixed] * 2,
        out_specs=(vmem, pl.BlockSpec(memory_space=pltpu.SMEM)),
        scratch_shapes=[
            pltpu.VMEM((depth, 2, 2, 2, rows, features), BF16),
            pltpu.VMEM((depth, 2, 2, 2, rows, features), BF16),
            pltpu.VMEM((2, count, features), BF16),
            pltpu.VMEM((count, depth * chunk), BF16),
            pltpu.VMEM((2, count, features), BF16),
            pltpu.VMEM((2, 8, count), F32),
            pltpu.VMEM((2, depth, 4 * rows, count), F32),
            pltpu.VMEM((2, depth, 4 * rows, count), F32),
            pltpu.VMEM((4 * rows, 2 * count), BF16),
            pltpu.VMEM((dp, seqs, features), BF16),
            pltpu.VMEM((dp, seqs, LANES), jnp.int32),
            pltpu.VMEM((padded, features), F32),
            pltpu.VMEM((padded, LANES), jnp.int32),
            pltpu.VMEM((depth, 2, 2, rows, half), BF16),
            pltpu.VMEM((depth, 2, 2, rows, half), BF16),
            pltpu.VMEM((depth, 2, 2, rows, half), F32),
            pltpu.VMEM((depth, 2, rows, half), BF16),
            pltpu.VMEM((depth, 2, rows, half), BF16),
            pltpu.VMEM((depth, 2, rows, half), F32),
            pltpu.VMEM((depth, rows, features), BF16),
            pltpu.VMEM((depth, rows, features), BF16),
            pltpu.VMEM((2, 1, LANES), F32),
            pltpu.SMEM((1, pairs), jnp.int32), pltpu.SMEM((pairs, hard), jnp.int32),
            dma((4,)), dma((2, depth)),
            dma((3,)), dma((3,)), dma((1,)), dma((1,)), dma((1,)), dma((1,)),
            dma((1,)), dma((1,)),
            dma((2,)), dma((depth, strips, 2)), dma((2,)), dma((depth, strips, 2)),
            dma((1,)), dma((1,)),
        ],
        compiler_params=pltpu.CompilerParams(
            collective_id=0, has_side_effects=True, vmem_limit_bytes=60 * 1024 * 1024
        ),
    )(
        q_hidden.reshape(pairs * length, features),
        p_hidden.reshape(pairs * length, features),
        arrange(w_up),
        arrange(w_down),
        pos_index.reshape(1, pairs),
        hard_index.reshape(pairs, hard),
    )
    return grad[:own_rows], loss.reshape(())


def solution(mesh):
    return jax.shard_map(
        functools.partial(shards, mesh.shape["dp"], mesh.shape["rep"]),
        mesh=mesh,
        in_specs=(
            P("rep", "dp", None, None),
            P("rep", "dp", None, None),
            P(),
            P(),
            P("rep", "dp"),
            P("rep", "dp", None),
        ),
        out_specs=(P(("dp", "rep"), None), P()),
        check_vma=False,
    )
```

```python
import functools
import math

import jax
import jax.numpy as jnp
from jax import lax
from jax.experimental import pallas as pl
from jax.experimental.pallas import tpu as pltpu
from jax.sharding import PartitionSpec as P

norm_eps = 1e-06
HARD_BOOST = 1.5
MESH = pl.DeviceIdType.MESH
LANES = 128
ROW_TILE = 16
LAGS = (6, 5)
F32 = jnp.float32
BF16 = jnp.bfloat16


def dot_nt(left, right):
    return lax.dot_general(
        left, right, (((1,), (1,)), ((), ())), preferred_element_type=F32
    )


def phi(values):
    return 0.5 * (1.0 + lax.erf(values * (1.0 / math.sqrt(2.0))))


def loop(count, body):
    if count <= 16:
        for step in range(count):
            body(step)
    else:
        lax.fori_loop(0, count, lambda step, carry: (body(step), carry)[1], 0)


def pipeline(tasks):
    cuts = sorted({edge - offset for _, first, last, offset in tasks for edge in (first, last)})
    for low, high in zip(cuts[:-1], cuts[1:]):
        active = [
            (body, offset) for body, first, last, offset in tasks
            if first <= low + offset and high + offset <= last
        ]

        def step_body(step, low=low, active=active):
            for body, offset in active:
                body(low + step + offset)

        loop(high - low, step_body)


def kernel(
    dp, pairs, length, hard,
    q_ref, p_ref, up_ref, down_ref, pos_ref, hard_ref,
    out_ref, loss_ref,
    up, down, tokens, normed, scales, slope, mixed, grads, slots, every, index_rows,
    first_out, first_in, first_kept, second_out, second_in, second_kept, z_out, z_in, losses,
    pos_smem, hard_smem, t_sem, w_sem, d_send, d_recv, e_send, e_recv,
    l_send, l_recv, first_send, first_recv, second_send, second_recv, z_send, z_recv,
):
    depth = dp // 4
    seqs = 2 * pairs
    count = seqs * length
    features = tokens.shape[-1]
    half = features // 2
    rows = up.shape[-2]
    block = 4 * rows
    chunk = 8 * rows
    strips = rows // ROW_TILE
    padded = every.shape[0]
    me = lax.axis_index("dp")
    my_rep = lax.axis_index("rep")
    other_rep = 1 - my_rep
    core = lax.rem(me, 2)
    side = lax.rem(me // 2, 2)
    layer = me // 4
    partner = me + 1 - 2 * core
    opposite = me + 2 - 4 * side

    def remote(src, dst, send, recv, device):
        return pltpu.make_async_remote_copy(
            src_ref=src, dst_ref=dst, send_sem=send, recv_sem=recv,
            device_id=device, device_id_type=MESH,
        )

    def ahead(step):
        return lax.rem(me + step, dp)

    half_count = pairs * length
    load_q = pltpu.make_async_copy(q_ref, tokens.at[core, pl.ds(0, half_count)], t_sem.at[0])
    load_p = pltpu.make_async_copy(p_ref, tokens.at[core, pl.ds(half_count, half_count)], t_sem.at[1])
    load_q.start()
    load_p.start()
    load_pos = pltpu.make_async_copy(pos_ref, pos_smem, t_sem.at[2])
    load_hard = pltpu.make_async_copy(hard_ref, hard_smem, t_sem.at[3])

    def load(which, step):
        ref, buffer = ((up_ref, up), (down_ref, down))[which]
        return pltpu.make_async_copy(ref.at[step], buffer.at[step], w_sem.at[which, step])

    loop(depth, lambda step: load(0, step).start())
    loop(depth, lambda step: load(1, step).start())
    load_pos.start()
    load_hard.start()

    barrier = pltpu.get_barrier_semaphore()

    def greet(step):
        pl.semaphore_signal(
            barrier, inc=1, device_id=(ahead(step + 1), my_rep), device_id_type=MESH
        )

    loop(dp - 1, greet)
    pl.semaphore_signal(barrier, inc=1, device_id=(me, other_rep), device_id_type=MESH)

    every[...] = jnp.zeros_like(every)
    index_rows[...] = jnp.full(index_rows.shape, -1.0, F32)

    load_q.wait()
    load_p.wait()
    own = tokens[core]

    load_pos.wait()
    load_hard.wait()
    row_ids = lax.broadcasted_iota(jnp.int32, (seqs, LANES), 0)
    lane_ids = lax.broadcasted_iota(jnp.int32, (seqs, LANES), 1)
    message = jnp.full((seqs, LANES), -1, jnp.int32)
    for row in range(pairs):
        message = jnp.where((row_ids == row) & (lane_ids == 0), pos_smem[0, row], message)
        for pick in range(hard):
            message = jnp.where(
                (row_ids == row) & (lane_ids == 1 + pick), hard_smem[row, pick], message
            )
    slots[me, :, features:] = message.astype(F32).astype(BF16)

    halves = (slice(0, depth // 2), slice(depth // 2, depth))

    def gelu_of(part):
        pre = dot_nt(own, up[part].reshape(-1, features))
        return (pre * phi(pre)).astype(BF16)

    loop(depth, lambda step: load(0, step).wait())
    loop(depth, lambda step: load(1, step).wait())
    lows = [gelu_of(part) for part in halves]
    summed = own.astype(F32)
    for part, low_part in zip(halves, lows):
        summed += jnp.dot(
            low_part, down[part].reshape(-1, features), preferred_element_type=F32
        )

    means, units, scale_list = [], [], []
    for seq in range(seqs):
        place = pl.ds(seq * length, length)
        part = summed[seq * length:(seq + 1) * length]
        centred = part - jnp.mean(part, -1, keepdims=True)
        scale = lax.rsqrt(jnp.mean(centred * centred, -1, keepdims=True) + norm_eps)
        unit = centred * scale
        units.append(unit)
        scale_list.append(scale)
        means.append(jnp.mean(unit, 0, keepdims=True))
    slots[me, :, :features] = jnp.concatenate(means, 0).astype(BF16)

    pl.semaphore_wait(barrier, dp)

    def embed_copy(step):
        return remote(
            slots.at[me], slots.at[me], e_send.at[0], e_recv.at[0],
            (ahead(step + 1), my_rep),
        )

    loop(dp - 1, lambda step: embed_copy(step).start())

    for seq in range(seqs):
        place = pl.ds(seq * length, length)
        normed[core, place, :] = units[seq].astype(BF16)
        scales[core, :, place] = jnp.broadcast_to(scale_list[seq], (length, LANES)).T[0:8]

    def twin_copy(which, slot):
        ref = (tokens, normed, scales)[which].at[slot]
        return remote(ref, ref, d_send.at[which], d_recv.at[which], (partner, my_rep))

    for which in range(3):
        twin_copy(which, core).start()

    def mix(step, slot):
        pre = dot_nt(up[step, :, core].reshape(block, features), tokens[slot])
        bell = jnp.exp(-0.5 * pre * pre) * (1.0 / math.sqrt(2.0 * math.pi))
        slope[slot, step] = (phi(pre) + pre * bell) * scales[slot][0:1]
        mixed[slot, step] = dot_nt(down[step, :, core].reshape(block, features), normed[slot])

    loop(depth, lambda step: mix(step, core))
    for which in range(3):
        twin_copy(which, 1 - core).wait_recv()
    loop(depth, lambda step: mix(step, 1 - core))

    def all_embeds():
        landed = slots.at[pl.ds(0, dp - 1)]
        return remote(landed, landed, e_send.at[0], e_recv.at[0], (me, my_rep))

    all_embeds().wait_recv()
    for slot in range(dp):
        every[slot * seqs:(slot + 1) * seqs, :] = slots[slot, :, :features].astype(F32)
        index_rows[slot * seqs:(slot + 1) * seqs, :] = slots[slot, :, features:].astype(F32)

    embeds = every[...].astype(BF16)
    scores = dot_nt(embeds, embeds)
    row = lax.broadcasted_iota(jnp.int32, (padded, padded), 0)
    column = lax.broadcasted_iota(jnp.int32, (padded, padded), 1)
    row_place = lax.rem(row, seqs)
    column_place = lax.rem(column, seqs)
    valid = (
        (row < dp * seqs) & (row_place < pairs) & (column < dp * seqs) & (column_place >= pairs)
    )
    passage = (column // seqs) * pairs + column_place - pairs
    indices = index_rows[...].astype(jnp.int32)
    target = valid & (passage == indices[:, 0:1])
    is_hard = passage == indices[:, 1:2]
    for pick in range(1, hard):
        is_hard = is_hard | (passage == indices[:, 1 + pick:2 + pick])
    logits = scores + jnp.where(is_hard, HARD_BOOST, 0.0)
    row_max = jnp.max(jnp.where(valid, logits, -1e30), -1, keepdims=True)
    powers = jnp.where(valid, jnp.exp(jnp.where(valid, logits - row_max, 0.0)), 0.0)
    powers_sum = jnp.sum(powers, -1, keepdims=True)
    log_total = row_max + jnp.log(jnp.where(powers_sum > 0.0, powers_sum, 1.0))
    picked = jnp.sum(jnp.where(target, logits, 0.0), -1, keepdims=True)
    weights = jnp.where(
        valid,
        jnp.exp(jnp.where(valid, logits - log_total, 0.0)) - jnp.where(target, 1.0, 0.0),
        0.0,
    )
    both = weights + weights.T
    chip_seqs = 2 * seqs
    first_row = (me - core) * seqs
    chip_weights = jnp.concatenate(
        [
            jnp.sum(jnp.where(row == first_row + seq, both, 0.0), 0, keepdims=True)
            for seq in range(chip_seqs)
        ]
        + [jnp.zeros((-chip_seqs % 8, padded), F32)] * (1 if chip_seqs % 8 else 0),
        0,
    ).astype(BF16)
    d_chip = jnp.dot(chip_weights, embeds, preferred_element_type=F32) * (1.0 / length)
    d_low = (d_chip - jnp.mean(d_chip, -1, keepdims=True)).astype(BF16)
    aligned = [dot_nt(d_low, normed[slot]) * (1.0 / features) for slot in range(2)]
    row_one = lax.broadcasted_iota(jnp.int32, (padded, 1), 0)
    counted = (row_one < dp * seqs) & (lax.rem(row_one, seqs) < pairs)
    loss = jnp.sum(jnp.where(counted, log_total - picked, 0.0), 0, keepdims=True)
    losses[my_rep] = jnp.broadcast_to(loss, (1, LANES))

    def loss_copy(group):
        return remote(
            losses.at[group], losses.at[group], l_send.at[0], l_recv.at[0], (me, other_rep)
        )

    def strip(sub):
        return pl.ds(sub * ROW_TILE, ROW_TILE)

    def turn(step):
        short = jnp.minimum(layer, depth - 1 - layer)
        ahead_first = jnp.where(2 * layer < depth, 1, -1)
        lone = depth - 1 - 2 * short
        late = jnp.maximum(step - lone, 0)
        return jnp.where(
            step < lone,
            layer + ahead_first * (depth - 1 - short - step),
            layer + ahead_first * (short - late // 2) * (2 * lax.rem(late, 2) - 1),
        )

    def place_of(index):
        if strips == 1:
            return turn(index), 0
        return turn(index // strips), index % strips

    low, high = slice(0, half), slice(half, features)

    def backward(step):
        now = turn(step)
        spread = dot_nt(down[now, :, core].reshape(block, features), d_low)
        for slot in range(2):
            for seq in range(seqs):
                which = slot * seqs + seq
                place = slice(seq * length, (seq + 1) * length)
                grads[:, slot * count + seq * length:slot * count + (seq + 1) * length] = (
                    slope[slot, now, :, place]
                    * (
                        spread[:, which:which + 1]
                        - aligned[slot][which:which + 1, place] * mixed[slot, now, :, place]
                    )
                ).astype(BF16)
        total = jnp.dot(
            grads[...], tokens[...].reshape(2 * count, features), preferred_element_type=F32
        ).reshape(2, 2, rows, features)
        by_side = [total[0, :, :, high], total[1, :, :, high]]
        by_rep = [total[:, 0, :, low], total[:, 1, :, low]]
        mine = (my_rep == 0)
        first_out[now, 0] = jnp.where(mine, by_rep[1], by_rep[0]).astype(BF16)
        first_kept[now, 0] = jnp.where(mine, by_rep[0], by_rep[1])
        mine = (side == 0)
        first_out[now, 1] = jnp.where(mine, by_side[1], by_side[0]).astype(BF16)
        first_kept[now, 1] = jnp.where(mine, by_side[0], by_side[1])

    across = ((me, other_rep), (opposite, my_rep))

    def first_copy(now, sub, way):
        return remote(
            first_out.at[now, way, :, strip(sub)], first_in.at[now, way, :, strip(sub)],
            first_send.at[way], first_recv.at[now, sub, way], across[way],
        )

    def second_copy(now, sub, way):
        return remote(
            second_out.at[now, way, strip(sub)], second_in.at[now, way, strip(sub)],
            second_send.at[way], second_recv.at[now, sub, way], across[1 - way],
        )

    def z_copy(now, sub):
        return remote(
            z_out.at[now, strip(sub)], z_in.at[layer, strip(sub)],
            z_send.at[0], z_recv.at[0],
            (now * 4 + side * 2 + core, my_rep),
        )

    def send_first(index):
        now, sub = place_of(index)
        for way in range(2):
            first_copy(now, sub, way).start()

    def stage_two(index):
        now, sub = place_of(index)
        for way in range(2):
            stays = (side, my_rep)[way]
            first_copy(now, sub, way).wait_recv()
            second_out[now, way, strip(sub), :] = (
                first_kept[now, way, 1 - stays, strip(sub), :]
                + first_in[now, way, 1 - stays, strip(sub), :].astype(F32)
            ).astype(BF16)
            second_copy(now, sub, way).start()
            second_kept[now, way, strip(sub), :] = (
                first_kept[now, way, stays, strip(sub), :]
                + first_in[now, way, stays, strip(sub), :].astype(F32)
            )

    def stage_three(index, last):
        now, sub = place_of(index)
        for way in range(2):
            second_copy(now, sub, way).wait_recv()
            total = second_kept[now, way, strip(sub), :] + second_in[now, way, strip(sub), :].astype(F32)
            if last:
                out_ref[strip(sub), (low, high)[way]] = total
            else:
                z_out[now, strip(sub), (low, high)[way]] = total.astype(BF16)
        if not last:
            z_copy(now, sub).start()

    steps = depth * strips
    moved = steps - strips
    lag_one, lag_two = LAGS
    early = min(depth, lag_one // strips)
    sent = min(steps, lag_one)

    def backward_and_send(step):
        backward(step)

        @pl.when(core == 0)
        def send_now():
            for sub in range(strips):
                send_first(step * strips + sub)

    loop(early, backward_and_send)
    loss_copy(my_rep).start()
    loop(depth - early, lambda step: backward(step + early))

    @pl.when(core != 0)
    def send_later():
        loop(early * strips, send_first)

    loop(sent - early * strips, lambda step: send_first(early * strips + step))
    pipeline([
        (send_first, sent, steps, sent),
        (stage_two, 0, steps, 0),
        (lambda index: stage_three(index, False), 0, moved, -lag_two),
        (lambda index: stage_three(index, True), moved, steps, -lag_two),
    ])

    def all_layers():
        landed = z_in.at[pl.ds(0, depth - 1)]
        return remote(landed, landed, z_send.at[0], z_recv.at[0], (opposite, my_rep))

    loss_copy(other_rep).wait_recv()
    loss_ref[0, 0] = (losses[0] + losses[1])[0, 0] * (1.0 / (dp * pairs * 2))
    all_layers().wait_recv()

    def collect(step):
        source = lax.rem(layer + depth - 1 - step, depth)
        out_ref[...] += z_in[source].astype(F32)

    loop(depth - 1, collect)

    all_embeds().wait_send()
    for which in range(3):
        twin_copy(which, core).wait_send()
    loss_copy(my_rep).wait_send()
    for way in range(2):
        sent_first = first_out.at[:, way]
        remote(sent_first, sent_first, first_send.at[way], first_recv.at[0, 0, way], across[way]).wait_send()
        sent_second = second_out.at[:, way]
        remote(sent_second, sent_second, second_send.at[way], second_recv.at[0, 0, way], across[1 - way]).wait_send()
    all_layers().wait_send()


def shards(dp, rep, q_hidden, p_hidden, w_up, w_down, pos_index, hard_index):
    assert rep == 2 and dp % 4 == 0
    assert dp * q_hidden.shape[1] <= 256
    pairs, length, features = q_hidden.shape[1:]
    hard = hard_index.shape[-1]
    hidden_units = w_up.shape[0]
    own_rows = hidden_units // (dp * rep)
    rows = -(-own_rows // ROW_TILE) * ROW_TILE
    depth = dp // 4
    strips = rows // ROW_TILE
    seqs = 2 * pairs
    count = seqs * length
    padded = -(-dp * seqs // LANES) * LANES
    chunk = 8 * rows
    half = features // 2

    def arrange(weight):
        blocks = weight.reshape(dp * rep, own_rows, features)
        if rows != own_rows:
            blocks = jnp.pad(blocks, ((0, 0), (0, rows - own_rows), (0, 0)))
        return blocks.reshape(depth, 2, 2, 2, rows, features)

    dma = pltpu.SemaphoreType.DMA
    hbm = pl.BlockSpec(memory_space=pl.ANY)
    fixed = pl.BlockSpec(memory_space=pltpu.HBM)
    vmem = pl.BlockSpec(memory_space=pltpu.VMEM)
    grad, loss = pl.pallas_call(
        functools.partial(kernel, dp, pairs, length, hard),
        name="gradcache_step",
        out_shape=(
            pltpu.VMEM((rows, features), F32),
            pltpu.SMEM((1, 1), F32),
        ),
        in_specs=[hbm] * 4 + [fixed] * 2,
        out_specs=(vmem, pl.BlockSpec(memory_space=pltpu.SMEM)),
        scratch_shapes=[
            pltpu.VMEM((depth, 2, 2, 2, rows, features), BF16),
            pltpu.VMEM((depth, 2, 2, 2, rows, features), BF16),
            pltpu.VMEM((2, count, features), BF16),
            pltpu.VMEM((2, count, features), BF16),
            pltpu.VMEM((2, 8, count), F32),
            pltpu.VMEM((2, depth, 4 * rows, count), F32),
            pltpu.VMEM((2, depth, 4 * rows, count), F32),
            pltpu.VMEM((4 * rows, 2 * count), BF16),
            pltpu.VMEM((dp, seqs, features + LANES), BF16),
            pltpu.VMEM((padded, features), F32),
            pltpu.VMEM((padded, LANES), F32),
            pltpu.VMEM((depth, 2, 2, rows, half), BF16),
            pltpu.VMEM((depth, 2, 2, rows, half), BF16),
            pltpu.VMEM((depth, 2, 2, rows, half), F32),
            pltpu.VMEM((depth, 2, rows, half), BF16),
            pltpu.VMEM((depth, 2, rows, half), BF16),
            pltpu.VMEM((depth, 2, rows, half), F32),
            pltpu.VMEM((depth, rows, features), BF16),
            pltpu.VMEM((depth, rows, features), BF16),
            pltpu.VMEM((2, 1, LANES), F32),
            pltpu.SMEM((1, pairs), jnp.int32), pltpu.SMEM((pairs, hard), jnp.int32),
            dma((4,)), dma((2, depth)),
            dma((3,)), dma((3,)), dma((1,)), dma((1,)),
            dma((1,)), dma((1,)),
            dma((2,)), dma((depth, strips, 2)), dma((2,)), dma((depth, strips, 2)),
            dma((1,)), dma((1,)),
        ],
        compiler_params=pltpu.CompilerParams(
            collective_id=0, has_side_effects=True, vmem_limit_bytes=60 * 1024 * 1024
        ),
    )(
        q_hidden.reshape(pairs * length, features),
        p_hidden.reshape(pairs * length, features),
        arrange(w_up),
        arrange(w_down),
        pos_index.reshape(1, pairs),
        hard_index.reshape(pairs, hard),
    )
    return grad[:own_rows], loss.reshape(())


def solution(mesh):
    return jax.shard_map(
        functools.partial(shards, mesh.shape["dp"], mesh.shape["rep"]),
        mesh=mesh,
        in_specs=(
            P("rep", "dp", None, None),
            P("rep", "dp", None, None),
            P(),
            P(),
            P("rep", "dp"),
            P("rep", "dp", None),
        ),
        out_specs=(P(("dp", "rep"), None), P()),
        check_vma=False,
    )
```

```python
import functools
import math

import jax
import jax.numpy as jnp
from jax import lax
from jax.experimental import pallas as pl
from jax.experimental.pallas import tpu as pltpu
from jax.sharding import PartitionSpec as P

norm_eps = 1e-06
HARD_BOOST = 1.5
MESH = pl.DeviceIdType.MESH
LANES = 128
ROW_TILE = 16
LAGS = (6, 5)
F32 = jnp.float32
BF16 = jnp.bfloat16


def dot_nt(left, right):
    return lax.dot_general(
        left, right, (((1,), (1,)), ((), ())), preferred_element_type=F32
    )


def phi(values):
    return 0.5 * (1.0 + lax.erf(values * (1.0 / math.sqrt(2.0))))


def loop(count, body):
    if count <= 16:
        for step in range(count):
            body(step)
    else:
        lax.fori_loop(0, count, lambda step, carry: (body(step), carry)[1], 0)


def pipeline(tasks):
    cuts = sorted({edge - offset for _, first, last, offset in tasks for edge in (first, last)})
    for low, high in zip(cuts[:-1], cuts[1:]):
        active = [
            (body, offset) for body, first, last, offset in tasks
            if first <= low + offset and high + offset <= last
        ]

        def step_body(step, low=low, active=active):
            for body, offset in active:
                body(low + step + offset)

        loop(high - low, step_body)


def kernel(
    dp, pairs, length, hard,
    q_ref, p_ref, up_ref, down_ref, pos_ref, hard_ref,
    out_ref, loss_ref,
    up, down, tokens, normed, scales, slope, mixed, grads, slots, every, index_rows,
    first_out, first_in, first_kept, second_out, second_in, second_kept, z_out, z_in, losses,
    pos_smem, hard_smem, t_sem, w_sem, d_send, d_recv, e_send, e_recv,
    l_send, l_recv, first_send, first_recv, second_send, second_recv, z_send, z_recv,
):
    depth = dp // 4
    seqs = 2 * pairs
    count = seqs * length
    features = tokens.shape[-1]
    half = features // 2
    rows = up.shape[-2]
    block = 4 * rows
    chunk = 8 * rows
    strips = rows // ROW_TILE
    padded = every.shape[0]
    me = lax.axis_index("dp")
    my_rep = lax.axis_index("rep")
    other_rep = 1 - my_rep
    core = lax.rem(me, 2)
    side = lax.rem(me // 2, 2)
    layer = me // 4
    partner = me + 1 - 2 * core
    opposite = me + 2 - 4 * side

    def remote(src, dst, send, recv, device):
        return pltpu.make_async_remote_copy(
            src_ref=src, dst_ref=dst, send_sem=send, recv_sem=recv,
            device_id=device, device_id_type=MESH,
        )

    def ahead(step):
        return lax.rem(me + step, dp)

    half_count = pairs * length
    load_q = pltpu.make_async_copy(q_ref, tokens.at[core, pl.ds(0, half_count)], t_sem.at[0])
    load_p = pltpu.make_async_copy(p_ref, tokens.at[core, pl.ds(half_count, half_count)], t_sem.at[1])
    load_q.start()
    load_p.start()
    load_pos = pltpu.make_async_copy(pos_ref, pos_smem, t_sem.at[2])
    load_hard = pltpu.make_async_copy(hard_ref, hard_smem, t_sem.at[3])

    def load(which, step):
        ref, buffer = ((up_ref, up), (down_ref, down))[which]
        return pltpu.make_async_copy(ref.at[step], buffer.at[step], w_sem.at[which, step])

    loop(depth, lambda step: load(0, step).start())
    loop(depth, lambda step: load(1, step).start())
    load_pos.start()
    load_hard.start()

    barrier = pltpu.get_barrier_semaphore()

    def greet(step):
        pl.semaphore_signal(
            barrier, inc=1, device_id=(ahead(step + 1), my_rep), device_id_type=MESH
        )

    loop(dp - 1, greet)
    pl.semaphore_signal(barrier, inc=1, device_id=(me, other_rep), device_id_type=MESH)

    every[...] = jnp.zeros_like(every)
    index_rows[...] = jnp.full(index_rows.shape, -1.0, F32)

    load_q.wait()
    load_p.wait()
    own = tokens[core]

    load_pos.wait()
    load_hard.wait()
    row_ids = lax.broadcasted_iota(jnp.int32, (seqs, LANES), 0)
    lane_ids = lax.broadcasted_iota(jnp.int32, (seqs, LANES), 1)
    message = jnp.full((seqs, LANES), -1, jnp.int32)
    for row in range(pairs):
        message = jnp.where((row_ids == row) & (lane_ids == 0), pos_smem[0, row], message)
        for pick in range(hard):
            message = jnp.where(
                (row_ids == row) & (lane_ids == 1 + pick), hard_smem[row, pick], message
            )
    slots[me, :, features:] = message.astype(F32).astype(BF16)

    halves = (slice(0, depth // 2), slice(depth // 2, depth))

    def gelu_of(part):
        pre = dot_nt(own, up[part].reshape(-1, features))
        return (pre * phi(pre)).astype(BF16)

    loop(depth, lambda step: load(0, step).wait())
    loop(depth, lambda step: load(1, step).wait())
    lows = [gelu_of(part) for part in halves]
    summed = own.astype(F32)
    for part, low_part in zip(halves, lows):
        summed += jnp.dot(
            low_part, down[part].reshape(-1, features), preferred_element_type=F32
        )

    means, units, scale_list = [], [], []
    for seq in range(seqs):
        place = pl.ds(seq * length, length)
        part = summed[seq * length:(seq + 1) * length]
        centred = part - jnp.mean(part, -1, keepdims=True)
        scale = lax.rsqrt(jnp.mean(centred * centred, -1, keepdims=True) + norm_eps)
        unit = centred * scale
        units.append(unit)
        scale_list.append(scale)
        means.append(jnp.mean(unit, 0, keepdims=True))
    slots[me, :, :features] = jnp.concatenate(means, 0).astype(BF16)

    pl.semaphore_wait(barrier, dp)

    def embed_copy(step):
        return remote(
            slots.at[me], slots.at[me], e_send.at[0], e_recv.at[0],
            (ahead(step + 1), my_rep),
        )

    loop(dp - 1, lambda step: embed_copy(step).start())

    for seq in range(seqs):
        place = pl.ds(seq * length, length)
        normed[core, place, :] = units[seq].astype(BF16)
        scales[core, :, place] = jnp.broadcast_to(scale_list[seq], (length, LANES)).T[0:8]

    def twin_copy(which, slot):
        ref = (tokens, normed, scales)[which].at[slot]
        return remote(ref, ref, d_send.at[which], d_recv.at[which], (partner, my_rep))

    for which in range(3):
        twin_copy(which, core).start()

    def mix(step, slot):
        pre = dot_nt(up[step, :, core].reshape(block, features), tokens[slot])
        bell = jnp.exp(-0.5 * pre * pre) * (1.0 / math.sqrt(2.0 * math.pi))
        slope[slot, step] = (phi(pre) + pre * bell) * scales[slot][0:1]
        mixed[slot, step] = dot_nt(down[step, :, core].reshape(block, features), normed[slot])

    loop(depth, lambda step: mix(step, core))
    for which in range(3):
        twin_copy(which, 1 - core).wait_recv()
    loop(depth, lambda step: mix(step, 1 - core))

    def all_embeds():
        landed = slots.at[pl.ds(0, dp - 1)]
        return remote(landed, landed, e_send.at[0], e_recv.at[0], (me, my_rep))

    all_embeds().wait_recv()
    for slot in range(dp):
        every[slot * seqs:(slot + 1) * seqs, :] = slots[slot, :, :features].astype(F32)
        index_rows[slot * seqs:(slot + 1) * seqs, :] = slots[slot, :, features:].astype(F32)

    embeds = every[...].astype(BF16)
    scores = dot_nt(embeds, embeds)
    row = lax.broadcasted_iota(jnp.int32, (padded, padded), 0)
    column = lax.broadcasted_iota(jnp.int32, (padded, padded), 1)
    row_place = lax.rem(row, seqs)
    column_place = lax.rem(column, seqs)
    valid = (
        (row < dp * seqs) & (row_place < pairs) & (column < dp * seqs) & (column_place >= pairs)
    )
    passage = (column // seqs) * pairs + column_place - pairs
    indices = index_rows[...].astype(jnp.int32)
    target = valid & (passage == indices[:, 0:1])
    is_hard = passage == indices[:, 1:2]
    for pick in range(1, hard):
        is_hard = is_hard | (passage == indices[:, 1 + pick:2 + pick])
    logits = scores + jnp.where(is_hard, HARD_BOOST, 0.0)
    row_max = jnp.max(jnp.where(valid, logits, -1e30), -1, keepdims=True)
    powers = jnp.where(valid, jnp.exp(jnp.where(valid, logits - row_max, 0.0)), 0.0)
    powers_sum = jnp.sum(powers, -1, keepdims=True)
    log_total = row_max + jnp.log(jnp.where(powers_sum > 0.0, powers_sum, 1.0))
    picked = jnp.sum(jnp.where(target, logits, 0.0), -1, keepdims=True)
    weights = jnp.where(
        valid,
        jnp.exp(jnp.where(valid, logits - log_total, 0.0)) - jnp.where(target, 1.0, 0.0),
        0.0,
    )
    both = weights + weights.T
    chip_seqs = 2 * seqs
    first_row = (me - core) * seqs
    chip_weights = jnp.concatenate(
        [
            jnp.sum(jnp.where(row == first_row + seq, both, 0.0), 0, keepdims=True)
            for seq in range(chip_seqs)
        ]
        + [jnp.zeros((-chip_seqs % 8, padded), F32)] * (1 if chip_seqs % 8 else 0),
        0,
    ).astype(BF16)
    d_chip = jnp.dot(chip_weights, embeds, preferred_element_type=F32) * (1.0 / length)
    d_low = (d_chip - jnp.mean(d_chip, -1, keepdims=True)).astype(BF16)
    aligned = [dot_nt(d_low, normed[slot]) * (1.0 / features) for slot in range(2)]
    row_one = lax.broadcasted_iota(jnp.int32, (padded, 1), 0)
    counted = (row_one < dp * seqs) & (lax.rem(row_one, seqs) < pairs)
    loss = jnp.sum(jnp.where(counted, log_total - picked, 0.0), 0, keepdims=True)
    losses[my_rep] = jnp.broadcast_to(loss, (1, LANES))

    def loss_copy(group):
        return remote(
            losses.at[group], losses.at[group], l_send.at[0], l_recv.at[0], (me, other_rep)
        )

    def strip(sub):
        return pl.ds(sub * ROW_TILE, ROW_TILE)

    def turn(step):
        short = jnp.minimum(layer, depth - 1 - layer)
        ahead_first = jnp.where(2 * layer < depth, 1, -1)
        lone = depth - 1 - 2 * short
        late = jnp.maximum(step - lone, 0)
        return jnp.where(
            step < lone,
            layer + ahead_first * (depth - 1 - short - step),
            layer + ahead_first * (short - late // 2) * (2 * lax.rem(late, 2) - 1),
        )

    def place_of(index):
        if strips == 1:
            return turn(index), 0
        return turn(index // strips), index % strips

    low, high = slice(0, half), slice(half, features)

    def backward(step):
        now = turn(step)
        spread = dot_nt(down[now, :, core].reshape(block, features), d_low)
        for slot in range(2):
            for seq in range(seqs):
                which = slot * seqs + seq
                place = slice(seq * length, (seq + 1) * length)
                grads[:, slot * count + seq * length:slot * count + (seq + 1) * length] = (
                    slope[slot, now, :, place]
                    * (
                        spread[:, which:which + 1]
                        - aligned[slot][which:which + 1, place] * mixed[slot, now, :, place]
                    )
                ).astype(BF16)
        total = jnp.dot(
            grads[...], tokens[...].reshape(2 * count, features), preferred_element_type=F32
        ).reshape(2, 2, rows, features)
        by_side = [total[0, :, :, high], total[1, :, :, high]]
        by_rep = [total[:, 0, :, low], total[:, 1, :, low]]
        mine = (my_rep == 0)
        first_out[now, 0] = jnp.where(mine, by_rep[1], by_rep[0]).astype(BF16)
        first_kept[now, 0] = jnp.where(mine, by_rep[0], by_rep[1])
        mine = (side == 0)
        first_out[now, 1] = jnp.where(mine, by_side[1], by_side[0]).astype(BF16)
        first_kept[now, 1] = jnp.where(mine, by_side[0], by_side[1])

    across = ((me, other_rep), (opposite, my_rep))

    def first_copy(now, sub, way):
        return remote(
            first_out.at[now, way, :, strip(sub)], first_in.at[now, way, :, strip(sub)],
            first_send.at[way], first_recv.at[now, sub, way], across[way],
        )

    def second_copy(now, sub, way):
        return remote(
            second_out.at[now, way, strip(sub)], second_in.at[now, way, strip(sub)],
            second_send.at[way], second_recv.at[now, sub, way], across[1 - way],
        )

    def z_copy(now, sub):
        return remote(
            z_out.at[now, strip(sub)], z_in.at[layer, strip(sub)],
            z_send.at[0], z_recv.at[0],
            (now * 4 + side * 2 + core, my_rep),
        )

    def send_first(index):
        now, sub = place_of(index)
        for way in range(2):
            first_copy(now, sub, way).start()

    def stage_two(index):
        now, sub = place_of(index)
        for way in range(2):
            stays = (side, my_rep)[way]
            first_copy(now, sub, way).wait_recv()
            second_out[now, way, strip(sub), :] = (
                first_kept[now, way, 1 - stays, strip(sub), :]
                + first_in[now, way, 1 - stays, strip(sub), :].astype(F32)
            ).astype(BF16)
            second_copy(now, sub, way).start()
            second_kept[now, way, strip(sub), :] = (
                first_kept[now, way, stays, strip(sub), :]
                + first_in[now, way, stays, strip(sub), :].astype(F32)
            )

    def stage_three(index, last):
        now, sub = place_of(index)
        for way in range(2):
            second_copy(now, sub, way).wait_recv()
            total = second_kept[now, way, strip(sub), :] + second_in[now, way, strip(sub), :].astype(F32)
            if last:
                out_ref[strip(sub), (low, high)[way]] = total
            else:
                z_out[now, strip(sub), (low, high)[way]] = total.astype(BF16)
        if not last:
            z_copy(now, sub).start()

    steps = depth * strips
    moved = steps - strips
    lag_one, lag_two = LAGS
    early = min(depth, lag_one // strips)
    sent = min(steps, lag_one)

    def backward_and_send(step):
        backward(step)

        @pl.when(core == 0)
        def send_now():
            for sub in range(strips):
                send_first(step * strips + sub)

    loop(early, backward_and_send)
    loss_copy(my_rep).start()
    loop(depth - early, lambda step: backward(step + early))

    @pl.when(core != 0)
    def send_later():
        loop(early * strips, send_first)

    loop(sent - early * strips, lambda step: send_first(early * strips + step))
    def finish_loss(index):
        loss_copy(other_rep).wait_recv()
        loss_ref[0, 0] = (losses[0] + losses[1])[0, 0] * (1.0 / (dp * pairs * 2))

    pipeline([
        (stage_two, 0, steps, 0),
        (send_first, sent, steps, sent),
        (finish_loss, 0, 1, -lag_two),
        (lambda index: stage_three(index, False), 0, moved, -lag_two),
        (lambda index: stage_three(index, True), moved, steps, -lag_two),
    ])

    def all_layers():
        landed = z_in.at[pl.ds(0, depth - 1)]
        return remote(landed, landed, z_send.at[0], z_recv.at[0], (opposite, my_rep))

    all_layers().wait_recv()

    def arrived(step):
        return z_in[lax.rem(layer + depth - 1 - step, depth)].astype(F32)

    if depth <= 16:
        out_ref[...] += sum(arrived(step) for step in range(depth - 1))
    else:
        def collect(step):
            out_ref[...] += arrived(step)

        loop(depth - 1, collect)

    all_embeds().wait_send()
    for which in range(3):
        twin_copy(which, core).wait_send()
    loss_copy(my_rep).wait_send()
    for way in range(2):
        sent_first = first_out.at[:, way]
        remote(sent_first, sent_first, first_send.at[way], first_recv.at[0, 0, way], across[way]).wait_send()
        sent_second = second_out.at[:, way]
        remote(sent_second, sent_second, second_send.at[way], second_recv.at[0, 0, way], across[1 - way]).wait_send()
    all_layers().wait_send()


def shards(dp, rep, q_hidden, p_hidden, w_up, w_down, pos_index, hard_index):
    assert rep == 2 and dp % 4 == 0
    assert dp * q_hidden.shape[1] <= 256
    pairs, length, features = q_hidden.shape[1:]
    hard = hard_index.shape[-1]
    hidden_units = w_up.shape[0]
    own_rows = hidden_units // (dp * rep)
    rows = -(-own_rows // ROW_TILE) * ROW_TILE
    depth = dp // 4
    strips = rows // ROW_TILE
    seqs = 2 * pairs
    count = seqs * length
    padded = -(-dp * seqs // LANES) * LANES
    chunk = 8 * rows
    half = features // 2

    def arrange(weight):
        blocks = weight.reshape(dp * rep, own_rows, features)
        if rows != own_rows:
            blocks = jnp.pad(blocks, ((0, 0), (0, rows - own_rows), (0, 0)))
        return blocks.reshape(depth, 2, 2, 2, rows, features)

    dma = pltpu.SemaphoreType.DMA
    hbm = pl.BlockSpec(memory_space=pl.ANY)
    fixed = pl.BlockSpec(memory_space=pltpu.HBM)
    vmem = pl.BlockSpec(memory_space=pltpu.VMEM)
    grad, loss = pl.pallas_call(
        functools.partial(kernel, dp, pairs, length, hard),
        name="gradcache_step",
        out_shape=(
            pltpu.VMEM((rows, features), F32),
            pltpu.SMEM((1, 1), F32),
        ),
        in_specs=[hbm] * 4 + [fixed] * 2,
        out_specs=(vmem, pl.BlockSpec(memory_space=pltpu.SMEM)),
        scratch_shapes=[
            pltpu.VMEM((depth, 2, 2, 2, rows, features), BF16),
            pltpu.VMEM((depth, 2, 2, 2, rows, features), BF16),
            pltpu.VMEM((2, count, features), BF16),
            pltpu.VMEM((2, count, features), BF16),
            pltpu.VMEM((2, 8, count), F32),
            pltpu.VMEM((2, depth, 4 * rows, count), F32),
            pltpu.VMEM((2, depth, 4 * rows, count), F32),
            pltpu.VMEM((4 * rows, 2 * count), BF16),
            pltpu.VMEM((dp, seqs, features + LANES), BF16),
            pltpu.VMEM((padded, features), F32),
            pltpu.VMEM((padded, LANES), F32),
            pltpu.VMEM((depth, 2, 2, rows, half), BF16),
            pltpu.VMEM((depth, 2, 2, rows, half), BF16),
            pltpu.VMEM((depth, 2, 2, rows, half), F32),
            pltpu.VMEM((depth, 2, rows, half), BF16),
            pltpu.VMEM((depth, 2, rows, half), BF16),
            pltpu.VMEM((depth, 2, rows, half), F32),
            pltpu.VMEM((depth, rows, features), BF16),
            pltpu.VMEM((depth, rows, features), BF16),
            pltpu.VMEM((2, 1, LANES), F32),
            pltpu.SMEM((1, pairs), jnp.int32), pltpu.SMEM((pairs, hard), jnp.int32),
            dma((4,)), dma((2, depth)),
            dma((3,)), dma((3,)), dma((1,)), dma((1,)),
            dma((1,)), dma((1,)),
            dma((2,)), dma((depth, strips, 2)), dma((2,)), dma((depth, strips, 2)),
            dma((1,)), dma((1,)),
        ],
        compiler_params=pltpu.CompilerParams(
            collective_id=0, has_side_effects=True, vmem_limit_bytes=60 * 1024 * 1024
        ),
    )(
        q_hidden.reshape(pairs * length, features),
        p_hidden.reshape(pairs * length, features),
        arrange(w_up),
        arrange(w_down),
        pos_index.reshape(1, pairs),
        hard_index.reshape(pairs, hard),
    )
    return grad[:own_rows], loss.reshape(())


def solution(mesh):
    return jax.shard_map(
        functools.partial(shards, mesh.shape["dp"], mesh.shape["rep"]),
        mesh=mesh,
        in_specs=(
            P("rep", "dp", None, None),
            P("rep", "dp", None, None),
            P(),
            P(),
            P("rep", "dp"),
            P("rep", "dp", None),
        ),
        out_specs=(P(("dp", "rep"), None), P()),
        check_vma=False,
    )
```

```python
import functools
import math

import jax
import jax.numpy as jnp
from jax import lax
from jax.experimental import pallas as pl
from jax.experimental.pallas import tpu as pltpu
from jax.sharding import PartitionSpec as P

norm_eps = 1e-06
HARD_BOOST = 1.5
MESH = pl.DeviceIdType.MESH
LANES = 128
ROW_TILE = 16
LAGS = (6, 5)
F32 = jnp.float32
BF16 = jnp.bfloat16


def dot_nt(left, right):
    return lax.dot_general(
        left, right, (((1,), (1,)), ((), ())), preferred_element_type=F32
    )


def phi(values):
    return 0.5 * (1.0 + lax.erf(values * (1.0 / math.sqrt(2.0))))


def loop(count, body):
    if count <= 16:
        for step in range(count):
            body(step)
    else:
        lax.fori_loop(0, count, lambda step, carry: (body(step), carry)[1], 0)


def pipeline(tasks):
    cuts = sorted({edge - offset for _, first, last, offset in tasks for edge in (first, last)})
    for low, high in zip(cuts[:-1], cuts[1:]):
        active = [
            (body, offset) for body, first, last, offset in tasks
            if first <= low + offset and high + offset <= last
        ]

        def step_body(step, low=low, active=active):
            for body, offset in active:
                body(low + step + offset)

        loop(high - low, step_body)


def kernel(
    dp, pairs, length, hard,
    q_ref, p_ref, up_ref, down_ref, pos_ref, hard_ref,
    out_ref, loss_ref,
    up, down, tokens, normed, scales, slope, mixed, grads, slots, every, index_rows,
    first_out, first_in, first_kept, second_out, second_in, second_kept, z_out, z_in, losses,
    pos_smem, hard_smem, t_sem, w_sem, d_send, d_recv, e_send, e_recv,
    l_send, l_recv, first_send, first_recv, second_send, second_recv, z_send, z_recv,
):
    depth = dp // 4
    seqs = 2 * pairs
    count = seqs * length
    features = tokens.shape[-1]
    half = features // 2
    rows = up.shape[-2]
    block = 4 * rows
    chunk = 8 * rows
    strips = rows // ROW_TILE
    padded = every.shape[0]
    me = lax.axis_index("dp")
    my_rep = lax.axis_index("rep")
    other_rep = 1 - my_rep
    core = lax.rem(me, 2)
    side = lax.rem(me // 2, 2)
    layer = me // 4
    partner = me + 1 - 2 * core
    opposite = me + 2 - 4 * side

    def remote(src, dst, send, recv, device):
        return pltpu.make_async_remote_copy(
            src_ref=src, dst_ref=dst, send_sem=send, recv_sem=recv,
            device_id=device, device_id_type=MESH,
        )

    def ahead(step):
        return lax.rem(me + step, dp)

    half_count = pairs * length
    load_q = pltpu.make_async_copy(q_ref, tokens.at[core, pl.ds(0, half_count)], t_sem.at[0])
    load_p = pltpu.make_async_copy(p_ref, tokens.at[core, pl.ds(half_count, half_count)], t_sem.at[1])
    load_q.start()
    load_p.start()
    load_pos = pltpu.make_async_copy(pos_ref, pos_smem, t_sem.at[2])
    load_hard = pltpu.make_async_copy(hard_ref, hard_smem, t_sem.at[3])

    def load(which, step):
        ref, buffer = ((up_ref, up), (down_ref, down))[which]
        return pltpu.make_async_copy(ref.at[step], buffer.at[step], w_sem.at[which, step])

    loop(depth, lambda step: load(0, step).start())
    loop(depth, lambda step: load(1, step).start())
    load_pos.start()
    load_hard.start()

    barrier = pltpu.get_barrier_semaphore()

    def greet(step):
        pl.semaphore_signal(
            barrier, inc=1, device_id=(ahead(step + 1), my_rep), device_id_type=MESH
        )

    loop(dp - 1, greet)
    pl.semaphore_signal(barrier, inc=1, device_id=(me, other_rep), device_id_type=MESH)

    every[...] = jnp.zeros_like(every)
    index_rows[...] = jnp.full(index_rows.shape, -1.0, F32)

    load_q.wait()
    load_p.wait()
    own = tokens[core]

    load_pos.wait()
    load_hard.wait()
    row_ids = lax.broadcasted_iota(jnp.int32, (seqs, LANES), 0)
    lane_ids = lax.broadcasted_iota(jnp.int32, (seqs, LANES), 1)
    message = jnp.full((seqs, LANES), -1, jnp.int32)
    for row in range(pairs):
        message = jnp.where((row_ids == row) & (lane_ids == 0), pos_smem[0, row], message)
        for pick in range(hard):
            message = jnp.where(
                (row_ids == row) & (lane_ids == 1 + pick), hard_smem[row, pick], message
            )
    slots[me, :, features:] = message.astype(F32).astype(BF16)

    halves = (slice(0, depth // 2), slice(depth // 2, depth))

    def up_of(part):
        return dot_nt(own, up[part].reshape(-1, features))

    loop(depth, lambda step: load(0, step).wait())
    loop(depth, lambda step: load(1, step).wait())
    pres = [up_of(part) for part in halves]
    summed = own.astype(F32)
    for part, pre in zip(halves, pres):
        low_part = (pre * phi(pre)).astype(BF16)
        summed += jnp.dot(
            low_part, down[part].reshape(-1, features), preferred_element_type=F32
        )

    means, units, scale_list = [], [], []
    for seq in range(seqs):
        place = pl.ds(seq * length, length)
        part = summed[seq * length:(seq + 1) * length]
        centred = part - jnp.mean(part, -1, keepdims=True)
        scale = lax.rsqrt(jnp.mean(centred * centred, -1, keepdims=True) + norm_eps)
        unit = centred * scale
        units.append(unit)
        scale_list.append(scale)
        means.append(jnp.mean(unit, 0, keepdims=True))
    slots[me, :, :features] = jnp.concatenate(means, 0).astype(BF16)

    pl.semaphore_wait(barrier, dp)

    def embed_copy(step):
        return remote(
            slots.at[me], slots.at[me], e_send.at[0], e_recv.at[0],
            (ahead(step + 1), my_rep),
        )

    loop(dp - 1, lambda step: embed_copy(step).start())

    for seq in range(seqs):
        place = pl.ds(seq * length, length)
        normed[core, place, :] = units[seq].astype(BF16)
        scales[core, :, place] = jnp.broadcast_to(scale_list[seq], (length, LANES)).T[0:8]

    def twin_copy(which, slot):
        ref = (tokens, normed, scales)[which].at[slot]
        return remote(ref, ref, d_send.at[which], d_recv.at[which], (partner, my_rep))

    for which in range(3):
        twin_copy(which, core).start()

    def mix(step, slot):
        pre = dot_nt(up[step, :, core].reshape(block, features), tokens[slot])
        bell = jnp.exp(-0.5 * pre * pre) * (1.0 / math.sqrt(2.0 * math.pi))
        slope[slot, step] = (phi(pre) + pre * bell) * scales[slot][0:1]
        mixed[slot, step] = dot_nt(down[step, :, core].reshape(block, features), normed[slot])

    loop(depth, lambda step: mix(step, core))
    for which in range(3):
        twin_copy(which, 1 - core).wait_recv()
    loop(depth, lambda step: mix(step, 1 - core))

    def all_embeds():
        landed = slots.at[pl.ds(0, dp - 1)]
        return remote(landed, landed, e_send.at[0], e_recv.at[0], (me, my_rep))

    all_embeds().wait_recv()
    for slot in range(dp):
        every[slot * seqs:(slot + 1) * seqs, :] = slots[slot, :, :features].astype(F32)
        index_rows[slot * seqs:(slot + 1) * seqs, :] = slots[slot, :, features:].astype(F32)

    embeds = every[...].astype(BF16)
    scores = dot_nt(embeds, embeds)
    row = lax.broadcasted_iota(jnp.int32, (padded, padded), 0)
    column = lax.broadcasted_iota(jnp.int32, (padded, padded), 1)
    row_place = lax.rem(row, seqs)
    column_place = lax.rem(column, seqs)
    valid = (
        (row < dp * seqs) & (row_place < pairs) & (column < dp * seqs) & (column_place >= pairs)
    )
    passage = (column // seqs) * pairs + column_place - pairs
    indices = index_rows[...].astype(jnp.int32)
    target = valid & (passage == indices[:, 0:1])
    is_hard = passage == indices[:, 1:2]
    for pick in range(1, hard):
        is_hard = is_hard | (passage == indices[:, 1 + pick:2 + pick])
    logits = scores + jnp.where(is_hard, HARD_BOOST, 0.0)
    row_max = jnp.max(jnp.where(valid, logits, -1e30), -1, keepdims=True)
    powers = jnp.where(valid, jnp.exp(jnp.where(valid, logits - row_max, 0.0)), 0.0)
    powers_sum = jnp.sum(powers, -1, keepdims=True)
    log_total = row_max + jnp.log(jnp.where(powers_sum > 0.0, powers_sum, 1.0))
    picked = jnp.sum(jnp.where(target, logits, 0.0), -1, keepdims=True)
    weights = jnp.where(
        valid,
        jnp.exp(jnp.where(valid, logits - log_total, 0.0)) - jnp.where(target, 1.0, 0.0),
        0.0,
    )
    both = weights + weights.T
    chip_seqs = 2 * seqs
    first_row = (me - core) * seqs
    chip_weights = jnp.concatenate(
        [
            jnp.sum(jnp.where(row == first_row + seq, both, 0.0), 0, keepdims=True)
            for seq in range(chip_seqs)
        ]
        + [jnp.zeros((-chip_seqs % 8, padded), F32)] * (1 if chip_seqs % 8 else 0),
        0,
    ).astype(BF16)
    d_chip = jnp.dot(chip_weights, embeds, preferred_element_type=F32) * (1.0 / length)
    d_low = (d_chip - jnp.mean(d_chip, -1, keepdims=True)).astype(BF16)
    aligned = [dot_nt(d_low, normed[slot]) * (1.0 / features) for slot in range(2)]
    row_one = lax.broadcasted_iota(jnp.int32, (padded, 1), 0)
    counted = (row_one < dp * seqs) & (lax.rem(row_one, seqs) < pairs)
    loss = jnp.sum(jnp.where(counted, log_total - picked, 0.0), 0, keepdims=True)
    losses[my_rep] = jnp.broadcast_to(loss, (1, LANES))

    def loss_copy(group):
        return remote(
            losses.at[group], losses.at[group], l_send.at[0], l_recv.at[0], (me, other_rep)
        )

    def strip(sub):
        return pl.ds(sub * ROW_TILE, ROW_TILE)

    def turn(step):
        short = jnp.minimum(layer, depth - 1 - layer)
        ahead_first = jnp.where(2 * layer < depth, 1, -1)
        lone = depth - 1 - 2 * short
        late = jnp.maximum(step - lone, 0)
        return jnp.where(
            step < lone,
            layer + ahead_first * (depth - 1 - short - step),
            layer + ahead_first * (short - late // 2) * (2 * lax.rem(late, 2) - 1),
        )

    def place_of(index):
        if strips == 1:
            return turn(index), 0
        return turn(index // strips), index % strips

    low, high = slice(0, half), slice(half, features)

    def backward(step):
        now = turn(step)
        spread = dot_nt(down[now, :, core].reshape(block, features), d_low)
        for slot in range(2):
            for seq in range(seqs):
                which = slot * seqs + seq
                place = slice(seq * length, (seq + 1) * length)
                grads[:, slot * count + seq * length:slot * count + (seq + 1) * length] = (
                    slope[slot, now, :, place]
                    * (
                        spread[:, which:which + 1]
                        - aligned[slot][which:which + 1, place] * mixed[slot, now, :, place]
                    )
                ).astype(BF16)
        total = jnp.dot(
            grads[...], tokens[...].reshape(2 * count, features), preferred_element_type=F32
        ).reshape(2, 2, rows, features)
        by_side = [total[0, :, :, high], total[1, :, :, high]]
        by_rep = [total[:, 0, :, low], total[:, 1, :, low]]
        mine = (my_rep == 0)
        first_out[now, 0] = jnp.where(mine, by_rep[1], by_rep[0]).astype(BF16)
        first_kept[now, 0] = jnp.where(mine, by_rep[0], by_rep[1])
        mine = (side == 0)
        first_out[now, 1] = jnp.where(mine, by_side[1], by_side[0]).astype(BF16)
        first_kept[now, 1] = jnp.where(mine, by_side[0], by_side[1])

    across = ((me, other_rep), (opposite, my_rep))

    def first_copy(now, sub, way):
        return remote(
            first_out.at[now, way, :, strip(sub)], first_in.at[now, way, :, strip(sub)],
            first_send.at[way], first_recv.at[now, sub, way], across[way],
        )

    def second_copy(now, sub, way):
        return remote(
            second_out.at[now, way, strip(sub)], second_in.at[now, way, strip(sub)],
            second_send.at[way], second_recv.at[now, sub, way], across[1 - way],
        )

    def z_copy(now, sub):
        return remote(
            z_out.at[now, strip(sub)], z_in.at[layer, strip(sub)],
            z_send.at[0], z_recv.at[0],
            (now * 4 + side * 2 + core, my_rep),
        )

    def send_first(index):
        now, sub = place_of(index)
        for way in range(2):
            first_copy(now, sub, way).start()

    def stage_two(index):
        now, sub = place_of(index)
        for way in range(2):
            stays = (side, my_rep)[way]
            first_copy(now, sub, way).wait_recv()
            second_out[now, way, strip(sub), :] = (
                first_kept[now, way, 1 - stays, strip(sub), :]
                + first_in[now, way, 1 - stays, strip(sub), :].astype(F32)
            ).astype(BF16)
            second_copy(now, sub, way).start()
            second_kept[now, way, strip(sub), :] = (
                first_kept[now, way, stays, strip(sub), :]
                + first_in[now, way, stays, strip(sub), :].astype(F32)
            )

    def stage_three(index, last):
        now, sub = place_of(index)
        for way in range(2):
            second_copy(now, sub, way).wait_recv()
            total = second_kept[now, way, strip(sub), :] + second_in[now, way, strip(sub), :].astype(F32)
            if last:
                out_ref[strip(sub), (low, high)[way]] = total
            else:
                z_out[now, strip(sub), (low, high)[way]] = total.astype(BF16)
        if not last:
            z_copy(now, sub).start()

    steps = depth * strips
    moved = steps - strips
    lag_one, lag_two = LAGS
    early = min(depth, lag_one // strips)
    sent = min(steps, lag_one)

    def backward_and_send(step):
        backward(step)

        @pl.when(core == 0)
        def send_now():
            for sub in range(strips):
                send_first(step * strips + sub)

    loop(early, backward_and_send)
    loss_copy(my_rep).start()
    loop(depth - early, lambda step: backward(step + early))

    @pl.when(core != 0)
    def send_later():
        loop(early * strips, send_first)

    loop(sent - early * strips, lambda step: send_first(early * strips + step))
    pipeline([
        (send_first, sent, steps, sent),
        (stage_two, 0, steps, 0),
        (lambda index: stage_three(index, False), 0, moved, -lag_two),
        (lambda index: stage_three(index, True), moved, steps, -lag_two),
    ])

    def all_layers():
        landed = z_in.at[pl.ds(0, depth - 1)]
        return remote(landed, landed, z_send.at[0], z_recv.at[0], (opposite, my_rep))

    loss_copy(other_rep).wait_recv()
    loss_ref[0, 0] = (losses[0] + losses[1])[0, 0] * (1.0 / (dp * pairs * 2))
    all_layers().wait_recv()

    def collect(step):
        source = lax.rem(layer + depth - 1 - step, depth)
        out_ref[...] += z_in[source].astype(F32)

    loop(depth - 1, collect)

    all_embeds().wait_send()
    for which in range(3):
        twin_copy(which, core).wait_send()
    loss_copy(my_rep).wait_send()
    for way in range(2):
        sent_first = first_out.at[:, way]
        remote(sent_first, sent_first, first_send.at[way], first_recv.at[0, 0, way], across[way]).wait_send()
        sent_second = second_out.at[:, way]
        remote(sent_second, sent_second, second_send.at[way], second_recv.at[0, 0, way], across[1 - way]).wait_send()
    all_layers().wait_send()


def shards(dp, rep, q_hidden, p_hidden, w_up, w_down, pos_index, hard_index):
    assert rep == 2 and dp % 4 == 0
    assert dp * q_hidden.shape[1] <= 256
    pairs, length, features = q_hidden.shape[1:]
    hard = hard_index.shape[-1]
    hidden_units = w_up.shape[0]
    own_rows = hidden_units // (dp * rep)
    rows = -(-own_rows // ROW_TILE) * ROW_TILE
    depth = dp // 4
    strips = rows // ROW_TILE
    seqs = 2 * pairs
    count = seqs * length
    padded = -(-dp * seqs // LANES) * LANES
    chunk = 8 * rows
    half = features // 2

    def arrange(weight):
        blocks = weight.reshape(dp * rep, own_rows, features)
        if rows != own_rows:
            blocks = jnp.pad(blocks, ((0, 0), (0, rows - own_rows), (0, 0)))
        return blocks.reshape(depth, 2, 2, 2, rows, features)

    dma = pltpu.SemaphoreType.DMA
    hbm = pl.BlockSpec(memory_space=pl.ANY)
    fixed = pl.BlockSpec(memory_space=pltpu.HBM)
    vmem = pl.BlockSpec(memory_space=pltpu.VMEM)
    grad, loss = pl.pallas_call(
        functools.partial(kernel, dp, pairs, length, hard),
        name="gradcache_step",
        out_shape=(
            pltpu.VMEM((rows, features), F32),
            pltpu.SMEM((1, 1), F32),
        ),
        in_specs=[hbm] * 4 + [fixed] * 2,
        out_specs=(vmem, pl.BlockSpec(memory_space=pltpu.SMEM)),
        scratch_shapes=[
            pltpu.VMEM((depth, 2, 2, 2, rows, features), BF16),
            pltpu.VMEM((depth, 2, 2, 2, rows, features), BF16),
            pltpu.VMEM((2, count, features), BF16),
            pltpu.VMEM((2, count, features), BF16),
            pltpu.VMEM((2, 8, count), F32),
            pltpu.VMEM((2, depth, 4 * rows, count), F32),
            pltpu.VMEM((2, depth, 4 * rows, count), F32),
            pltpu.VMEM((4 * rows, 2 * count), BF16),
            pltpu.VMEM((dp, seqs, features + LANES), BF16),
            pltpu.VMEM((padded, features), F32),
            pltpu.VMEM((padded, LANES), F32),
            pltpu.VMEM((depth, 2, 2, rows, half), BF16),
            pltpu.VMEM((depth, 2, 2, rows, half), BF16),
            pltpu.VMEM((depth, 2, 2, rows, half), F32),
            pltpu.VMEM((depth, 2, rows, half), BF16),
            pltpu.VMEM((depth, 2, rows, half), BF16),
            pltpu.VMEM((depth, 2, rows, half), F32),
            pltpu.VMEM((depth, rows, features), BF16),
            pltpu.VMEM((depth, rows, features), BF16),
            pltpu.VMEM((2, 1, LANES), F32),
            pltpu.SMEM((1, pairs), jnp.int32), pltpu.SMEM((pairs, hard), jnp.int32),
            dma((4,)), dma((2, depth)),
            dma((3,)), dma((3,)), dma((1,)), dma((1,)),
            dma((1,)), dma((1,)),
            dma((2,)), dma((depth, strips, 2)), dma((2,)), dma((depth, strips, 2)),
            dma((1,)), dma((1,)),
        ],
        compiler_params=pltpu.CompilerParams(
            collective_id=0, has_side_effects=True, vmem_limit_bytes=60 * 1024 * 1024
        ),
    )(
        q_hidden.reshape(pairs * length, features),
        p_hidden.reshape(pairs * length, features),
        arrange(w_up),
        arrange(w_down),
        pos_index.reshape(1, pairs),
        hard_index.reshape(pairs, hard),
    )
    return grad[:own_rows], loss.reshape(())


def solution(mesh):
    return jax.shard_map(
        functools.partial(shards, mesh.shape["dp"], mesh.shape["rep"]),
        mesh=mesh,
        in_specs=(
            P("rep", "dp", None, None),
            P("rep", "dp", None, None),
            P(),
            P(),
            P("rep", "dp"),
            P("rep", "dp", None),
        ),
        out_specs=(P(("dp", "rep"), None), P()),
        check_vma=False,
    )
```
